128 devices in a mesh: replica: 1, data: 2 (over core), table: 64 (over z, y, x).
Axes of the slice: x: 4, y: 4, z: 4, core: 2. Of those that a mesh axis runs over, the one named last changes fastest.
Arguments:
- tokens: bfloat16 [65536, 1024], P(('replica', 'data', 'table'))
- grad_out: bfloat16 [65536, 1024], P(('replica', 'data', 'table'))
- table_u: bfloat16 [16384, 1024], P(('replica', 'table'))
- table_v: bfloat16 [16384, 1024], P(('replica', 'table'))
- wanted_ids: int32 [128, 8192], P(('replica', 'data', 'table'))
- pick_idx: int32 [65536, 8, 16], P(('replica', 'data', 'table'))
- gate_val: float32 [65536, 8, 16], P(('replica', 'data', 'table'))
Outputs:
- output 1: bfloat16 [65536, 1024], P(('replica', 'data', 'table'))
- output 2: bfloat16 [65536, 1024], P(('replica', 'data', 'table'))
- output 3: bfloat16 [16384, 1024], P(('replica', 'table'))
- output 4: bfloat16 [16384, 1024], P(('replica', 'table'))
All inputs are finite; a program needn't handle non-finite values.
Results may differ from the reference program's by a relative error of at most 0.00769059.
Values are sent between devices in bfloat16 or wider.
A program may use at most 1 GiB of HBM per device.

```python
import math
import jax
import jax.numpy as jnp
from jax import lax

D = 1024
N = 16384
HEADS = 8
TOPK = 16
TOK_DEV = 512
DATA = 2
TABLE = 64
POOL = 128

N_LOCAL = N // TABLE
DEVS = DATA * TABLE
T_PART = DEVS * TOK_DEV
SEL_TOK = HEADS * TOPK
SEL_DEV = TOK_DEV * SEL_TOK
ENTRIES = TABLE * POOL
BLOCK = math.gcd(TOK_DEV, max(1, 8192 // SEL_TOK))


def draw_routing(route_key):
    perm_key, off_key, own_key_a, own_key_b, slot_key, mix_key = jax.random.split(route_key, 6)
    orders = jax.vmap(lambda one_key: jax.random.permutation(one_key, N_LOCAL))(jax.random.split(perm_key, TABLE))
    offsets = jax.random.randint(off_key, (DEVS, TABLE, 1), 0, 2 * POOL)
    spot_idx = (offsets + jnp.arange(POOL, dtype=jnp.int32)[None, None, :]) % N_LOCAL
    owner_idx = jnp.arange(TABLE, dtype=jnp.int32)[None, :, None]
    local_rows = orders[owner_idx, spot_idx]
    wanted = (local_rows + owner_idx * N_LOCAL).reshape(DEVS, ENTRIES).astype(jnp.int32)
    extra_len = SEL_DEV - ENTRIES
    own_a = jax.random.randint(own_key_a, (DEVS, extra_len), 0, TABLE)
    own_b = jax.random.randint(own_key_b, (DEVS, extra_len), 0, TABLE)
    slot_idx = jax.random.randint(slot_key, (DEVS, extra_len), 0, POOL)
    extra_picks = jnp.minimum(own_a, own_b) * POOL + slot_idx
    cover = jnp.broadcast_to(jnp.arange(ENTRIES, dtype=jnp.int32)[None, :], (DEVS, ENTRIES))
    pick_all = jnp.concatenate([cover, extra_picks.astype(jnp.int32)], axis=1)
    shuffle = jax.vmap(lambda one_key: jax.random.permutation(one_key, SEL_DEV))(jax.random.split(mix_key, DEVS))
    pick_all = jnp.take_along_axis(pick_all, shuffle, axis=1)
    return wanted, pick_all.reshape(T_PART, HEADS, TOPK).astype(jnp.int32)


def setup_inputs(seed: int = 0, part: int = 0) -> dict:
    part_key = jax.random.fold_in(jax.random.key(seed), part)
    key_list = jax.random.split(part_key, 6)
    tokens = jax.random.normal(key_list[0], (T_PART, D), jnp.float32).astype(jnp.bfloat16)
    grad_out = jax.random.normal(key_list[1], (T_PART, D), jnp.float32).astype(jnp.bfloat16)
    table_u = (jax.random.normal(key_list[2], (N, D), jnp.float32) * D ** -0.5).astype(jnp.bfloat16)
    table_v = (jax.random.normal(key_list[3], (N, D), jnp.float32) * SEL_TOK ** -0.5).astype(jnp.bfloat16)
    wanted_ids, pick_idx = draw_routing(key_list[4])
    gate_val = jax.random.uniform(key_list[5], (T_PART, HEADS, TOPK), jnp.float32, 0.5, 1.5)
    return {'tokens': tokens, 'grad_out': grad_out, 'table_u': table_u, 'table_v': table_v, 'wanted_ids': wanted_ids, 'pick_idx': pick_idx, 'gate_val': gate_val}


def gelu_pair(pre_act):
    cdf_val = 0.5 * (1.0 + lax.erf(pre_act * 0.7071067811865476))
    pdf_val = jnp.exp(-0.5 * pre_act * pre_act) * 0.3989422804014327
    return pre_act * cdf_val, cdf_val + pre_act * pdf_val


def reference(tokens, grad_out, table_u, table_v, wanted_ids, pick_idx, gate_val):
    sel_ids = jnp.take_along_axis(wanted_ids, pick_idx.reshape(DEVS, SEL_DEV), axis=1)
    num_blocks = T_PART // BLOCK
    inputs = (tokens.reshape(num_blocks, BLOCK, D), grad_out.reshape(num_blocks, BLOCK, D), sel_ids.reshape(num_blocks, BLOCK, SEL_TOK), gate_val.reshape(num_blocks, BLOCK, SEL_TOK))

    def body(acc_pair, block_in):
        acc_u, acc_v = acc_pair
        x_blk, dy_blk, id_blk, gate_blk = block_in
        x_f = x_blk.astype(jnp.float32)
        dy_f = dy_blk.astype(jnp.float32)
        sel_u = jnp.take(table_u, id_blk, axis=0).astype(jnp.float32)
        sel_v = jnp.take(table_v, id_blk, axis=0).astype(jnp.float32)
        pre_act = jnp.einsum('bsd,bd->bs', sel_u, x_f)
        act_val, slope_val = gelu_pair(pre_act)
        weight = gate_blk * act_val
        y_blk = jnp.einsum('bs,bsd->bd', weight, sel_v)
        v_dot_dy = jnp.einsum('bsd,bd->bs', sel_v, dy_f)
        coef_sel = gate_blk * slope_val * v_dot_dy
        dx_blk = jnp.einsum('bs,bsd->bd', coef_sel, sel_u)
        flat_ids = id_blk.reshape(-1)
        acc_u = acc_u.at[flat_ids].add((coef_sel[:, :, None] * x_f[:, None, :]).reshape(-1, D))
        acc_v = acc_v.at[flat_ids].add((weight[:, :, None] * dy_f[:, None, :]).reshape(-1, D))
        return (acc_u, acc_v), (y_blk.astype(jnp.bfloat16), dx_blk.astype(jnp.bfloat16))

    zero_acc = jnp.zeros((N, D), jnp.float32)
    (acc_u, acc_v), (y_st, dx_st) = lax.scan(body, (zero_acc, zero_acc), inputs)
    return (y_st.reshape(T_PART, D), dx_st.reshape(T_PART, D), acc_u.astype(jnp.bfloat16), acc_v.astype(jnp.bfloat16))
```

```python
import functools
import jax
import jax.numpy as jnp
from jax import lax
from jax.experimental import pallas as pl
from jax.experimental.pallas import tpu as pltpu
from jax.sharding import PartitionSpec as P

F32 = jnp.float32
BF16 = jnp.bfloat16
SIDE = 4
OWN_STEP = 4
VMEM_LIMIT = 60 * 1024 * 1024
B_CALLS = 4
OUT_CALLS = 8
ROW_CUTS = (0, 48, 88, 128)
AXIS_ORDERS = ((2, 1, 0), (1, 0, 2), (0, 2, 1))


def split3(val):
    one = val.astype(BF16)
    rest = val - one.astype(F32)
    two = rest.astype(BF16)
    rest = rest - two.astype(F32)
    return one, two, rest.astype(BF16)


def dot_nn(lhs, rhs):
    return lax.dot_general(lhs, rhs, (((1,), (0,)), ((), ())), preferred_element_type=F32)


def dot_nt(lhs, rhs):
    return lax.dot_general(lhs, rhs, (((1,), (1,)), ((), ())), preferred_element_type=F32)


def swap_fields(val):
    return val ^ ((val & 21) << 1)


def gate_kernel(n_own, pick_ref, gate_ref, out_ref, tile_ref):
    sel = pick_ref.shape[1]
    iota_own = lax.broadcasted_iota(jnp.int32, (n_own, sel), 0)
    iota_lo = lax.broadcasted_iota(jnp.int32, (128, sel), 0)

    def body(grp, carry):
        base = pl.multiple_of(grp * 8, 8)
        pick = pick_ref[pl.ds(base, 8), :]
        hi = pick >> 7
        lo = pick & 127
        parts = [piece.astype(F32) for piece in split3(gate_ref[pl.ds(base, 8), :])]
        for j in range(8):
            mask = iota_own == hi[j:j + 1, :]
            left = jnp.concatenate([jnp.where(mask, piece[j:j + 1, :], 0.0).astype(BF16) for piece in parts], axis=0)
            right = jnp.where(iota_lo == lo[j:j + 1, :], 1.0, 0.0).astype(BF16)
            res = dot_nt(left, right)
            tile_ref[j * n_own:(j + 1) * n_own, :] = res[:n_own] + res[n_own:2 * n_own] + res[2 * n_own:]
        for o in range(n_own):
            out_ref[pl.ds(base, 8), o * 128:(o + 1) * 128] = tile_ref[pl.ds(o, 8, stride=n_own), :]
        return carry

    lax.fori_loop(0, pick_ref.shape[0] // 8, body, 0)


def gate_matrix(pick_rel, gate, n_own):
    tok, sel = pick_rel.shape
    blk = max(8, tok // 4)
    return pl.pallas_call(
        functools.partial(gate_kernel, n_own),
        grid=(tok // blk,),
        in_specs=[pl.BlockSpec((blk, sel), lambda i: (i, 0)), pl.BlockSpec((blk, sel), lambda i: (i, 0))],
        out_specs=pl.BlockSpec((blk, n_own * 128), lambda i: (i, 0)),
        out_shape=jax.ShapeDtypeStruct((tok, n_own * 128), F32),
        scratch_shapes=[pltpu.VMEM((8 * n_own, 128), F32)],
        compiler_params=pltpu.CompilerParams(vmem_limit_bytes=VMEM_LIMIT),
        cost_estimate=pl.CostEstimate(flops=2 * tok * 256 * 256 * 192, bytes_accessed=tok * n_own * 512, transcendentals=0),
        name="gate_matrix",
    )(pick_rel, gate)


def select_rows(xoff_ref, tab_ref, idsb_ref, sel_ref):
    n_rows = tab_ref.shape[0] // OWN_STEP
    iota = lax.broadcasted_iota(jnp.int32, (128, 128), 1)
    for j in range(OWN_STEP):
        ids = idsb_ref[j * 128:(j + 1) * 128, :]
        hot = jnp.concatenate([jnp.where(ids == iota + 128 * h, 1.0, 0.0).astype(BF16) for h in range(n_rows // 128)], axis=1)
        start = pl.multiple_of(xoff_ref[j] * n_rows, n_rows)
        sel_ref[j * 128:(j + 1) * 128, :] = dot_nn(hot, tab_ref[pl.ds(start, n_rows), :]).astype(BF16)


def place_rows(blk, grad_t, ids_ref, keep_ref, send_ref):
    iota = lax.broadcasted_iota(jnp.int32, (256, 128), 0)
    grad_b = grad_t.astype(BF16)
    for j in range(OWN_STEP):
        hot = jnp.where(iota == ids_ref[pl.ds(blk * OWN_STEP + j, 1), :], 1.0, 0.0).astype(BF16)
        rows = dot_nt(hot, grad_b[:, j * 128:(j + 1) * 128]).astype(BF16)
        keep_ref[j * 128:(j + 1) * 128, :] = rows[:128]
        k = swap_fields(j)
        send_ref[k * 128:(k + 1) * 128, :] = rows[128:]


def first_kernel(ublk_ref, xoff_ref, tok_ref, dyt_ref, tab_ref, idsb_ref, ids_ref, gate_ref, w_ref, slope_ref, sel_ref, keep_ref, send_ref):
    select_rows(xoff_ref, tab_ref, idsb_ref, sel_ref)
    pre = dot_nt(tok_ref[...], sel_ref[...])
    gate = gate_ref[...]
    cdf = 0.5 * (1.0 + lax.erf(pre * 0.7071067811865476))
    pdf = jnp.exp(-0.5 * pre * pre) * 0.3989422804014327
    live = gate != 0.0
    w = jnp.where(live, gate * (pre * cdf), 0.0)
    w_ref[...] = w
    slope_ref[...] = jnp.where(live, gate * (cdf + pre * pdf), 0.0)
    one, two, three = split3(w)
    dyt = dyt_ref[...]
    grad_t = dot_nn(dyt, one) + dot_nn(dyt, two) + dot_nn(dyt, three)
    place_rows(pl.program_id(0), grad_t, ids_ref, keep_ref, send_ref)


def first_pass(ublk, xoff, tok, dyt, table, idsb, ids_flip, gate):
    n_tok, width = tok.shape
    n_list = gate.shape[1]
    cols = OWN_STEP * 128
    steps = n_list // cols
    trows = table.shape[0] // steps
    row_blk = pl.BlockSpec((cols, width), lambda i, u, x: (i, 0))
    mat_blk = pl.BlockSpec((n_tok, cols), lambda i, u, x: (0, i))
    return pl.pallas_call(
        first_kernel,
        grid_spec=pltpu.PrefetchScalarGridSpec(
            num_scalar_prefetch=2,
            grid=(steps,),
            in_specs=[
                pl.BlockSpec((n_tok, width), lambda i, u, x: (0, 0)),
                pl.BlockSpec((width, n_tok), lambda i, u, x: (0, 0)),
                pl.BlockSpec((trows, width), lambda i, u, x: (u[i], 0)),
                pl.BlockSpec((cols, 128), lambda i, u, x: (i, 0)),
                pl.BlockSpec(ids_flip.shape, lambda i, u, x: (0, 0)),
                mat_blk,
            ],
            out_specs=[mat_blk, mat_blk, row_blk, row_blk, pl.BlockSpec((cols, width), lambda i, u, x: (swap_fields(i), 0))],
        ),
        out_shape=[
            jax.ShapeDtypeStruct((n_tok, n_list), F32),
            jax.ShapeDtypeStruct((n_tok, n_list), F32),
            jax.ShapeDtypeStruct((n_list, width), BF16),
            jax.ShapeDtypeStruct((n_list, width), BF16),
            jax.ShapeDtypeStruct((n_list, width), BF16),
        ],
        compiler_params=pltpu.CompilerParams(vmem_limit_bytes=VMEM_LIMIT),
        cost_estimate=pl.CostEstimate(flops=11 * n_tok * n_list * width, bytes_accessed=n_list * (width * 10 + n_tok * 12), transcendentals=0),
        name="first_pass",
    )(ublk, xoff, tok, dyt, table, idsb, ids_flip, gate)


def second_kernel(first_blk, n_alias, ublk_ref, xoff_ref, dy_ref, tokt_ref, tab_ref, idsb_ref, ids_ref, slope_ref, *rest):
    c_ref, sel_ref, keep_ref, send_ref = rest[n_alias:]
    select_rows(xoff_ref, tab_ref, idsb_ref, sel_ref)
    back = dot_nt(dy_ref[...], sel_ref[...])
    slope = slope_ref[...]
    c = jnp.where(slope != 0.0, slope * back, 0.0)
    c_ref[...] = c
    one, two, three = split3(c)
    tokt = tokt_ref[...]
    grad_t = dot_nn(tokt, one) + dot_nn(tokt, two) + dot_nn(tokt, three)
    place_rows(pl.program_id(0) + first_blk, grad_t, ids_ref, keep_ref, send_ref)


def second_pass(ublk, xoff, dy, tokt, table, idsb, ids_flip, slope):
    n_tok, width = dy.shape
    n_list = slope.shape[1]
    cols = OWN_STEP * 128
    steps = n_list // cols
    per = steps // B_CALLS
    trows = table.shape[0] // steps
    outs = []
    for call in range(B_CALLS):
        at = call * per
        row_blk = pl.BlockSpec((cols, width), lambda i, u, x, at=at: (i + at, 0))
        mat_blk = pl.BlockSpec((n_tok, cols), lambda i, u, x, at=at: (0, i + at))
        outs = pl.pallas_call(
            functools.partial(second_kernel, at, len(outs)),
            grid_spec=pltpu.PrefetchScalarGridSpec(
                num_scalar_prefetch=2,
                grid=(per,),
                in_specs=[
                    pl.BlockSpec((n_tok, width), lambda i, u, x: (0, 0)),
                    pl.BlockSpec((width, n_tok), lambda i, u, x: (0, 0)),
                    pl.BlockSpec((trows, width), lambda i, u, x, at=at: (u[i + at], 0)),
                    pl.BlockSpec((cols, 128), lambda i, u, x, at=at: (i + at, 0)),
                    pl.BlockSpec(ids_flip.shape, lambda i, u, x: (0, 0)),
                    mat_blk,
                ] + [pl.BlockSpec(memory_space=pl.ANY)] * len(outs),
                out_specs=[mat_blk, row_blk, row_blk, pl.BlockSpec((cols, width), lambda i, u, x, at=at: (swap_fields(i + at), 0))],
            ),
            out_shape=[
                jax.ShapeDtypeStruct((n_tok, n_list), F32),
                jax.ShapeDtypeStruct((n_list, width), BF16),
                jax.ShapeDtypeStruct((n_list, width), BF16),
                jax.ShapeDtypeStruct((n_list, width), BF16),
            ],
            input_output_aliases={8 + k: k for k in range(len(outs))},
            compiler_params=pltpu.CompilerParams(vmem_limit_bytes=VMEM_LIMIT),
            cost_estimate=pl.CostEstimate(flops=11 * n_tok * n_list * width // B_CALLS, bytes_accessed=n_list * (width * 10 + n_tok * 8) // B_CALLS, transcendentals=0),
            name="second_pass",
        )(ublk, xoff, dy, tokt, table, idsb, ids_flip, slope, *outs)
    return outs


def out_kernel(has_in, w_ref, c_ref, v_ref, u_ref, *rest):
    y_in, dx_in = rest[:2] if has_in else (None, None)
    y_ref, dx_ref, y_acc, dx_acc = rest[-4:]
    step = pl.program_id(0)

    @pl.when(step == 0)
    def _():
        y_acc[...] = y_in[...] if has_in else jnp.zeros_like(y_acc)
        dx_acc[...] = dx_in[...] if has_in else jnp.zeros_like(dx_acc)

    for mat_ref, row_ref, acc in ((w_ref, v_ref, y_acc), (c_ref, u_ref, dx_acc)):
        one, two, three = split3(mat_ref[...])
        rows = row_ref[...]
        acc[...] += dot_nn(one, rows) + dot_nn(two, rows) + dot_nn(three, rows)

    @pl.when(step == pl.num_programs(0) - 1)
    def _():
        y_ref[...] = y_acc[...].astype(y_ref.dtype)
        dx_ref[...] = dx_acc[...].astype(dx_ref.dtype)


def out_pass(w, c, v_sel, u_sel):
    n_tok, n_list = w.shape
    width = v_sel.shape[1]
    cols = OWN_STEP * 128
    per = n_list // cols // OUT_CALLS
    accs = []
    whole = pl.BlockSpec((n_tok, width), lambda i: (0, 0))
    for call in range(OUT_CALLS):
        at = call * per
        dtype = BF16 if call == OUT_CALLS - 1 else F32
        accs = pl.pallas_call(
            functools.partial(out_kernel, bool(accs)),
            grid=(per,),
            in_specs=[
                pl.BlockSpec((n_tok, cols), lambda i, at=at: (0, i + at)),
                pl.BlockSpec((n_tok, cols), lambda i, at=at: (0, i + at)),
                pl.BlockSpec((cols, width), lambda i, at=at: (i + at, 0)),
                pl.BlockSpec((cols, width), lambda i, at=at: (i + at, 0)),
            ] + [whole] * len(accs),
            out_specs=[whole, whole],
            out_shape=[jax.ShapeDtypeStruct((n_tok, width), dtype)] * 2,
            scratch_shapes=[pltpu.VMEM((n_tok, width), F32)] * 2,
            compiler_params=pltpu.CompilerParams(vmem_limit_bytes=VMEM_LIMIT),
            cost_estimate=pl.CostEstimate(flops=12 * n_tok * n_list * width // OUT_CALLS, bytes_accessed=n_list * (width * 4 + n_tok * 8) // OUT_CALLS, transcendentals=0),
            name="out_pass",
        )(w, c, v_sel, u_sel, *accs)
    return accs


def neighbour_pairs(field, step, table_n):
    pairs = []
    for core in range(2):
        flip = (1 if (core == 0) == (step == 0) else 3) << (2 * field)
        pairs += [(core * table_n + r, core * table_n + (r ^ flip)) for r in range(table_n)]
    return pairs


def halve_rows(keep, send, table_n):
    width = keep.shape[-1]
    axes = ('data', 'table')
    swap = [(i, (i + table_n) % (2 * table_n)) for i in range(2 * table_n)]
    got0 = lax.ppermute(send, axes, swap)
    cube = (SIDE, SIDE, SIDE, 128, width)
    keep, got0 = keep.reshape(cube), got0.reshape(cube)
    done = []
    for strm in range(3):
        cut = slice(ROW_CUTS[strm], ROW_CUTS[strm + 1])
        val = keep[:, :, :, cut].astype(F32) + got0[:, :, :, cut].astype(F32)
        left = [0, 1, 2]
        for axis in AXIS_ORDERS[strm]:
            dim = left.index(axis)
            left.remove(axis)
            field = 2 - axis
            take = lambda arr, lo, hi: lax.slice_in_dim(arr, lo, hi, axis=dim)
            got = lax.ppermute(take(val, 1, 3).astype(BF16), axes, neighbour_pairs(field, 0, table_n))
            far = take(val, 3, 4) + take(got, 1, 2).astype(F32)
            got2 = lax.ppermute(far.astype(BF16), axes, neighbour_pairs(field, 1, table_n))
            val = take(val, 0, 1) + take(got, 0, 1).astype(F32) + got2.astype(F32)
            val = val.reshape(val.shape[:dim] + val.shape[dim + 1:])
        done.append(val)
    mine = jnp.concatenate(done, axis=0).astype(BF16)
    return lax.all_gather(mine, 'data', axis=0, tiled=True)


def solution(mesh):
    table_n = mesh.shape['table']
    tok_spec = P(('replica', 'data', 'table'))
    row_spec = P(('replica', 'table'))

    def device_step(tok, dy, u_loc, v_loc, wanted, pick, gate):
        n_local, width = u_loc.shape
        half = n_local // 2
        n_tok = tok.shape[0]
        core = lax.axis_index('data')
        me = lax.axis_index('table')
        own_rows = lambda arr: lax.dynamic_slice_in_dim(arr, core * half, half, 0)
        full_u = lax.all_gather(own_rows(u_loc), ('table', 'data'), axis=0, tiled=True)
        full_v = lax.all_gather(own_rows(v_loc), ('table', 'data'), axis=0, tiled=True)

        slots = jnp.arange(table_n, dtype=jnp.int32)
        relabel = lambda val: jnp.where(core == 1, swap_fields(val), val)
        owners = relabel(slots) ^ me
        ublk = relabel(jnp.arange(table_n // OWN_STEP, dtype=jnp.int32)) ^ (me >> 2)
        xoff = relabel(jnp.arange(OWN_STEP, dtype=jnp.int32)) ^ (me & 3)
        ids = jnp.take(wanted.reshape(table_n, -1), owners, axis=0, mode='clip') - owners[:, None] * n_local
        ids_flip = ids ^ (core * half)
        idsb = jnp.broadcast_to(ids.reshape(-1, 1), (ids.size, 128))
        pick = pick.reshape(n_tok, -1)
        pick_rel = (relabel((pick >> 7) ^ me) << 7) | (pick & 127)
        gates = gate_matrix(pick_rel, gate.reshape(n_tok, -1), table_n)

        w, slope, u_sel, keep_v, send_v = first_pass(ublk, xoff, tok, dy.T, full_u, idsb, ids_flip, gates)
        grad_v = halve_rows(keep_v, send_v, table_n)
        c, v_sel, keep_u, send_u = second_pass(ublk, xoff, dy, tok.T, full_v, idsb, ids_flip, slope)
        grad_u = halve_rows(keep_u, send_u, table_n)
        y, dx = out_pass(w, c, v_sel, u_sel)
        return y, dx, grad_u, grad_v

    return jax.shard_map(device_step, mesh=mesh, in_specs=(tok_spec, tok_spec, row_spec, row_spec, tok_spec, tok_spec, tok_spec), out_specs=(tok_spec, tok_spec, row_spec, row_spec), check_vma=False)
```

```python
import functools
import jax
import jax.numpy as jnp
from jax import lax
from jax.experimental import pallas as pl
from jax.experimental.pallas import tpu as pltpu
from jax.sharding import PartitionSpec as P

F32 = jnp.float32
BF16 = jnp.bfloat16
SIDE = 4
OWN_STEP = 4
VMEM_LIMIT = 60 * 1024 * 1024
B_CALLS = 4
ROW_CUTS = (0, 48, 88, 128)
AXIS_ORDERS = ((2, 1, 0), (1, 0, 2), (0, 2, 1))


def split3(val):
    one = val.astype(BF16)
    rest = val - one.astype(F32)
    two = rest.astype(BF16)
    rest = rest - two.astype(F32)
    return one, two, rest.astype(BF16)


def dot_nn(lhs, rhs):
    return lax.dot_general(lhs, rhs, (((1,), (0,)), ((), ())), preferred_element_type=F32)


def dot_nt(lhs, rhs):
    return lax.dot_general(lhs, rhs, (((1,), (1,)), ((), ())), preferred_element_type=F32)


def swap_fields(val):
    return val ^ ((val & 21) << 1)


def gate_kernel(n_own, pick_ref, gate_ref, out_ref, tile_ref):
    sel = pick_ref.shape[1]
    iota_own = lax.broadcasted_iota(jnp.int32, (n_own, sel), 0)
    iota_lo = lax.broadcasted_iota(jnp.int32, (128, sel), 0)

    def body(grp, carry):
        base = pl.multiple_of(grp * 8, 8)
        pick = pick_ref[pl.ds(base, 8), :]
        hi = pick >> 7
        lo = pick & 127
        parts = [piece.astype(F32) for piece in split3(gate_ref[pl.ds(base, 8), :])]
        for j in range(8):
            mask = iota_own == hi[j:j + 1, :]
            left = jnp.concatenate([jnp.where(mask, piece[j:j + 1, :], 0.0).astype(BF16) for piece in parts], axis=0)
            right = jnp.where(iota_lo == lo[j:j + 1, :], 1.0, 0.0).astype(BF16)
            res = dot_nt(left, right)
            tile_ref[j * n_own:(j + 1) * n_own, :] = res[:n_own] + res[n_own:2 * n_own] + res[2 * n_own:]
        for o in range(n_own):
            out_ref[pl.ds(base, 8), o * 128:(o + 1) * 128] = tile_ref[pl.ds(o, 8, stride=n_own), :]
        return carry

    lax.fori_loop(0, pick_ref.shape[0] // 8, body, 0)


def gate_matrix(pick_rel, gate, n_own):
    tok, sel = pick_rel.shape
    blk = max(8, tok // 4)
    return pl.pallas_call(
        functools.partial(gate_kernel, n_own),
        grid=(tok // blk,),
        in_specs=[pl.BlockSpec((blk, sel), lambda i: (i, 0)), pl.BlockSpec((blk, sel), lambda i: (i, 0))],
        out_specs=pl.BlockSpec((blk, n_own * 128), lambda i: (i, 0)),
        out_shape=jax.ShapeDtypeStruct((tok, n_own * 128), F32),
        scratch_shapes=[pltpu.VMEM((8 * n_own, 128), F32)],
        compiler_params=pltpu.CompilerParams(vmem_limit_bytes=VMEM_LIMIT),
        cost_estimate=pl.CostEstimate(flops=2 * tok * 256 * 256 * 192, bytes_accessed=tok * n_own * 512, transcendentals=0),
        name="gate_matrix",
    )(pick_rel, gate)


def select_rows(xoff_ref, tab_ref, idsb_ref, sel_ref):
    n_rows = tab_ref.shape[0] // OWN_STEP
    iota = lax.broadcasted_iota(jnp.int32, (128, 128), 1)
    for j in range(OWN_STEP):
        ids = idsb_ref[j * 128:(j + 1) * 128, :]
        hot = jnp.concatenate([jnp.where(ids == iota + 128 * h, 1.0, 0.0).astype(BF16) for h in range(n_rows // 128)], axis=1)
        start = pl.multiple_of(xoff_ref[j] * n_rows, n_rows)
        sel_ref[j * 128:(j + 1) * 128, :] = dot_nn(hot, tab_ref[pl.ds(start, n_rows), :]).astype(BF16)


def place_rows(blk, grad_t, ids_ref, keep_ref, send_ref):
    iota = lax.broadcasted_iota(jnp.int32, (256, 128), 0)
    grad_b = grad_t.astype(BF16)
    for j in range(OWN_STEP):
        hot = jnp.where(iota == ids_ref[pl.ds(blk * OWN_STEP + j, 1), :], 1.0, 0.0).astype(BF16)
        rows = dot_nt(hot, grad_b[:, j * 128:(j + 1) * 128]).astype(BF16)
        keep_ref[j * 128:(j + 1) * 128, :] = rows[:128]
        k = swap_fields(j)
        send_ref[k * 128:(k + 1) * 128, :] = rows[128:]


def first_kernel(ublk_ref, xoff_ref, tok_ref, dyt_ref, tab_ref, idsb_ref, ids_ref, gate_ref, w_ref, slope_ref, sel_ref, keep_ref, send_ref):
    select_rows(xoff_ref, tab_ref, idsb_ref, sel_ref)
    pre = dot_nt(tok_ref[...], sel_ref[...])
    gate = gate_ref[...]
    cdf = 0.5 * (1.0 + lax.erf(pre * 0.7071067811865476))
    pdf = jnp.exp(-0.5 * pre * pre) * 0.3989422804014327
    live = gate != 0.0
    w = jnp.where(live, gate * (pre * cdf), 0.0)
    w_ref[...] = w
    slope_ref[...] = jnp.where(live, gate * (cdf + pre * pdf), 0.0)
    one, two, three = split3(w)
    dyt = dyt_ref[...]
    grad_t = dot_nn(dyt, one) + dot_nn(dyt, two) + dot_nn(dyt, three)
    place_rows(pl.program_id(0), grad_t, ids_ref, keep_ref, send_ref)


def first_pass(ublk, xoff, tok, dyt, table, idsb, ids_flip, gate):
    n_tok, width = tok.shape
    n_list = gate.shape[1]
    cols = OWN_STEP * 128
    steps = n_list // cols
    trows = table.shape[0] // steps
    row_blk = pl.BlockSpec((cols, width), lambda i, u, x: (i, 0))
    mat_blk = pl.BlockSpec((n_tok, cols), lambda i, u, x: (0, i))
    return pl.pallas_call(
        first_kernel,
        grid_spec=pltpu.PrefetchScalarGridSpec(
            num_scalar_prefetch=2,
            grid=(steps,),
            in_specs=[
                pl.BlockSpec((n_tok, width), lambda i, u, x: (0, 0)),
                pl.BlockSpec((width, n_tok), lambda i, u, x: (0, 0)),
                pl.BlockSpec((trows, width), lambda i, u, x: (u[i], 0)),
                pl.BlockSpec((cols, 128), lambda i, u, x: (i, 0)),
                pl.BlockSpec(ids_flip.shape, lambda i, u, x: (0, 0)),
                mat_blk,
            ],
            out_specs=[mat_blk, mat_blk, row_blk, row_blk, pl.BlockSpec((cols, width), lambda i, u, x: (swap_fields(i), 0))],
        ),
        out_shape=[
            jax.ShapeDtypeStruct((n_tok, n_list), F32),
            jax.ShapeDtypeStruct((n_tok, n_list), F32),
            jax.ShapeDtypeStruct((n_list, width), BF16),
            jax.ShapeDtypeStruct((n_list, width), BF16),
            jax.ShapeDtypeStruct((n_list, width), BF16),
        ],
        compiler_params=pltpu.CompilerParams(vmem_limit_bytes=VMEM_LIMIT),
        cost_estimate=pl.CostEstimate(flops=11 * n_tok * n_list * width, bytes_accessed=n_list * (width * 10 + n_tok * 12), transcendentals=0),
        name="first_pass",
    )(ublk, xoff, tok, dyt, table, idsb, ids_flip, gate)


def second_kernel(first_blk, n_alias, ublk_ref, xoff_ref, dy_ref, tokt_ref, tab_ref, idsb_ref, ids_ref, slope_ref, *rest):
    c_ref, sel_ref, keep_ref, send_ref, tok_ref = rest[n_alias:]
    select_rows(xoff_ref, tab_ref, idsb_ref, sel_ref)
    back = dot_nt(dy_ref[...], sel_ref[...])
    slope = slope_ref[...]
    c = jnp.where(slope != 0.0, slope * back, 0.0)
    c_ref[...] = c
    one, two, three = split3(c)
    tokt = tokt_ref[...]
    grad_t = dot_nn(tokt, one) + dot_nn(tokt, two) + dot_nn(tokt, three)
    place_rows(pl.program_id(0) + first_blk, grad_t, ids_ref, keep_ref, send_ref)
    tok_ref[...] = jnp.zeros_like(tok_ref)


def second_part(call, ublk, xoff, dy, tokt, table, idsb, ids_flip, slope, outs):
    n_tok, width = dy.shape
    n_list = slope.shape[1]
    cols = OWN_STEP * 128
    steps = n_list // cols
    per = steps // B_CALLS
    trows = table.shape[0] // steps
    at = call * per
    row_blk = pl.BlockSpec((cols, width), lambda i, u, x: (i + at, 0))
    mat_blk = pl.BlockSpec((n_tok, cols), lambda i, u, x: (0, i + at))
    return pl.pallas_call(
        functools.partial(second_kernel, at, len(outs)),
        grid_spec=pltpu.PrefetchScalarGridSpec(
            num_scalar_prefetch=2,
            grid=(per,),
            in_specs=[
                pl.BlockSpec((n_tok, width), lambda i, u, x: (0, 0)),
                pl.BlockSpec((width, n_tok), lambda i, u, x: (0, 0)),
                pl.BlockSpec((trows, width), lambda i, u, x: (u[i + at], 0)),
                pl.BlockSpec((cols, 128), lambda i, u, x: (i + at, 0)),
                pl.BlockSpec(ids_flip.shape, lambda i, u, x: (0, 0)),
                mat_blk,
            ] + [pl.BlockSpec(memory_space=pl.ANY)] * len(outs),
            out_specs=[mat_blk, row_blk, row_blk, pl.BlockSpec((cols, width), lambda i, u, x: (swap_fields(i + at), 0)), pl.BlockSpec((8, 128), lambda i, u, x: (0, 0))],
        ),
        out_shape=[
            jax.ShapeDtypeStruct((n_tok, n_list), F32),
            jax.ShapeDtypeStruct((n_list, width), BF16),
            jax.ShapeDtypeStruct((n_list, width), BF16),
            jax.ShapeDtypeStruct((n_list, width), BF16),
            jax.ShapeDtypeStruct((8, 128), F32),
        ],
        input_output_aliases={8 + k: k for k in range(len(outs))},
        compiler_params=pltpu.CompilerParams(vmem_limit_bytes=VMEM_LIMIT),
        cost_estimate=pl.CostEstimate(flops=11 * n_tok * n_list * width // B_CALLS, bytes_accessed=n_list * (width * 10 + n_tok * 8) // B_CALLS, transcendentals=0),
        name="second_pass",
    )(ublk, xoff, dy, tokt, table, idsb, ids_flip, slope, *outs)


def out_kernel(tie_ref, mat_ref, row_ref, out_ref, tok_ref, acc_ref):
    step = pl.program_id(0)
    one, two, three = split3(mat_ref[...])
    rows = row_ref[...]
    part = dot_nn(one, rows) + dot_nn(two, rows) + dot_nn(three, rows)

    @pl.when(step == 0)
    def _():
        acc_ref[...] = part
        tok_ref[...] = jnp.zeros_like(tok_ref)

    @pl.when(step > 0)
    def _():
        acc_ref[...] += part

    @pl.when(step == pl.num_programs(0) - 1)
    def _():
        out_ref[...] = acc_ref[...].astype(out_ref.dtype)


def out_half(tie, mat, rows, half):
    n_tok, n_list = mat.shape
    width = rows.shape[1] // 2
    cols = 1024
    return pl.pallas_call(
        out_kernel,
        grid_spec=pltpu.PrefetchScalarGridSpec(
            num_scalar_prefetch=1,
            grid=(n_list // cols,),
            in_specs=[
                pl.BlockSpec((n_tok, cols), lambda i, t: (0, i)),
                pl.BlockSpec((cols, width), lambda i, t: (i, half)),
            ],
            out_specs=[pl.BlockSpec((n_tok, width), lambda i, t: (0, 0)), pl.BlockSpec((8, 128), lambda i, t: (0, 0))],
            scratch_shapes=[pltpu.VMEM((n_tok, width), F32)],
        ),
        out_shape=[jax.ShapeDtypeStruct((n_tok, width), BF16), jax.ShapeDtypeStruct((8, 128), F32)],
        compiler_params=pltpu.CompilerParams(vmem_limit_bytes=VMEM_LIMIT),
        cost_estimate=pl.CostEstimate(flops=6 * n_tok * n_list * width, bytes_accessed=n_list * (width * 2 + n_tok * 4), transcendentals=0),
        name="out_half",
    )(tie, mat, rows)


def neighbour_pairs(field, step, table_n):
    pairs = []
    for core in range(2):
        flip = (1 if (core == 0) == (step == 0) else 3) << (2 * field)
        pairs += [(core * table_n + r, core * table_n + (r ^ flip)) for r in range(table_n)]
    return pairs


class HalveRows:
    def __init__(self, keep, send, table_n):
        self.table_n = table_n
        swap = [(i, (i + table_n) % (2 * table_n)) for i in range(2 * table_n)]
        self.keep = keep
        self.gots = [lax.ppermute(send, ('data', 'table'), swap)]
        self.stage = 0

    def tie(self, token):
        out = lax.optimization_barrier((token, *self.gots))
        self.gots = list(out[1:])

    def make_sends(self):
        if self.stage == 0:
            cube = (SIDE, SIDE, SIDE, 128, self.keep.shape[-1])
            pair = [self.keep.reshape(cube), self.gots[0].reshape(cube)]
            self.terms = [[arr[:, :, :, ROW_CUTS[k]:ROW_CUTS[k + 1]] for arr in pair] for k in range(3)]
            self.left = [[0, 1, 2] for _ in range(3)]
        sends = []
        for k in range(3):
            axis = AXIS_ORDERS[k][self.stage // 2]
            dim = self.left[k].index(axis)
            take = lambda arr, lo, hi: lax.slice_in_dim(arr, lo, hi, axis=dim)
            add = lambda arrs: functools.reduce(jnp.add, [arr.astype(F32) for arr in arrs]).astype(BF16)
            if self.stage % 2 == 0:
                if self.stage > 0:
                    prev = self.left_dim[k]
                    self.terms[k] = [t.reshape(t.shape[:prev] + t.shape[prev + 1:]) for t in self.kept[k] + [self.gots[k]]]
                    self.left[k].remove(AXIS_ORDERS[k][self.stage // 2 - 1])
                    dim = self.left[k].index(axis)
                sends.append(add([take(t, 1, 3) for t in self.terms[k]]))
            else:
                got = self.gots[k]
                sends.append(add([take(t, 3, 4) for t in self.terms[k]] + [take(got, 1, 2)]))
                if k == 0:
                    self.kept, self.left_dim = [], []
                self.kept.append([take(t, 0, 1) for t in self.terms[k]] + [take(got, 0, 1)])
                self.left_dim.append(dim)
        self.sends = sends

    def send(self):
        self.gots = [lax.ppermute(self.sends[k], ('data', 'table'), neighbour_pairs(2 - AXIS_ORDERS[k][self.stage // 2], self.stage % 2, self.table_n)) for k in range(3)]
        self.stage += 1

    def step(self, token=None, hold=None):
        if token is not None:
            self.tie(token)
        self.make_sends()
        if hold is not None:
            out = lax.optimization_barrier((hold, *self.sends))
            hold, self.sends = out[0], list(out[1:])
        self.send()
        return hold

    def finish(self):
        done = []
        for k in range(3):
            arrs = [t.reshape(t.shape[-2:]) for t in self.kept[k] + [self.gots[k]]]
            done.append(functools.reduce(jnp.add, [t.astype(F32) for t in arrs]))
        mine = jnp.concatenate(done, axis=0).astype(BF16)
        return lax.all_gather(mine, 'data', axis=0, tiled=True)


def solution(mesh):
    table_n = mesh.shape['table']
    tok_spec = P(('replica', 'data', 'table'))
    row_spec = P(('replica', 'table'))

    def device_step(tok, dy, u_loc, v_loc, wanted, pick, gate):
        n_local, width = u_loc.shape
        half = n_local // 2
        n_tok = tok.shape[0]
        core = lax.axis_index('data')
        me = lax.axis_index('table')
        own_rows = lambda arr: lax.dynamic_slice_in_dim(arr, core * half, half, 0)
        full_u = lax.all_gather(own_rows(u_loc), ('table', 'data'), axis=0, tiled=True)
        full_v = lax.all_gather(own_rows(v_loc), ('table', 'data'), axis=0, tiled=True)

        slots = jnp.arange(table_n, dtype=jnp.int32)
        relabel = lambda val: jnp.where(core == 1, swap_fields(val), val)
        owners = relabel(slots) ^ me
        ublk = relabel(jnp.arange(table_n // OWN_STEP, dtype=jnp.int32)) ^ (me >> 2)
        xoff = relabel(jnp.arange(OWN_STEP, dtype=jnp.int32)) ^ (me & 3)
        ids = jnp.take(wanted.reshape(table_n, -1), owners, axis=0, mode='clip') - owners[:, None] * n_local
        ids_flip = ids ^ (core * half)
        idsb = jnp.broadcast_to(ids.reshape(-1, 1), (ids.size, 128))
        pick = pick.reshape(n_tok, -1)
        pick_rel = (relabel((pick >> 7) ^ me) << 7) | (pick & 127)
        gates = gate_matrix(pick_rel, gate.reshape(n_tok, -1), table_n)

        w, slope, u_sel, keep_v, send_v = first_pass(ublk, xoff, tok, dy.T, full_u, idsb, ids_flip, gates)
        red_v = HalveRows(keep_v, send_v, table_n)
        tokt = tok.T
        outs, token = [], None
        for call in range(B_CALLS):
            tie = ublk
            if call != 1:
                tie = red_v.step(token, ublk)
            *outs, token = second_part(call, tie, xoff, dy, tokt, full_v, idsb, ids_flip, slope, outs)
        c, v_sel, keep_u, send_u = outs
        red_u = HalveRows(keep_u, send_u, table_n)
        tie = red_v.step(token, xoff)
        y0, token = out_half(tie, w, v_sel, 0)
        tie = red_v.step(token, xoff)
        y1, token = out_half(tie, w, v_sel, 1)
        tie = red_v.step(token, xoff)
        tie = red_u.step(token, tie)
        dx0, token = out_half(tie, c, u_sel, 0)
        red_v.tie(token)
        grad_v = red_v.finish()
        dx1, token = out_half(token[0, :4].astype(jnp.int32), c, u_sel, 1)
        red_u.step(token)
        for _ in range(4):
            red_u.step()
        grad_u = red_u.finish()
        y = jnp.concatenate([y0, y1], axis=1)
        dx = jnp.concatenate([dx0, dx1], axis=1)
        return y, dx, grad_u, grad_v

    return jax.shard_map(device_step, mesh=mesh, in_specs=(tok_spec, tok_spec, row_spec, row_spec, tok_spec, tok_spec, tok_spec), out_specs=(tok_spec, tok_spec, row_spec, row_spec), check_vma=False)
```

```python
import functools
import jax
import jax.numpy as jnp
from jax import lax
from jax.experimental import pallas as pl
from jax.experimental.pallas import tpu as pltpu
from jax.sharding import PartitionSpec as P

F32 = jnp.float32
BF16 = jnp.bfloat16
SIDE = 4
OWN_STEP = 4
VMEM_LIMIT = 60 * 1024 * 1024
ROW_CUTS = (0, 48, 88, 128)
AXIS_ORDERS = ((2, 1, 0), (1, 0, 2), (0, 2, 1))


def split3(val):
    one = val.astype(BF16)
    rest = val - one.astype(F32)
    two = rest.astype(BF16)
    rest = rest - two.astype(F32)
    return one, two, rest.astype(BF16)


def dot_nn(lhs, rhs):
    return lax.dot_general(lhs, rhs, (((1,), (0,)), ((), ())), preferred_element_type=F32)


def dot_nt(lhs, rhs):
    return lax.dot_general(lhs, rhs, (((1,), (1,)), ((), ())), preferred_element_type=F32)


def xor_field(val, other):
    return (val // 2 + other // 2) % 2 * 2 + (val % 2 + other % 2) % 2


def table_block(step):
    me = lax.axis_index('table')
    return xor_field(step // 4, me // 16) * 4 + xor_field(step % 4, (me // 4) % 4)


def gate_kernel(n_own, pick_ref, gate_ref, out_ref, tile_ref):
    sel = pick_ref.shape[1]
    iota_own = lax.broadcasted_iota(jnp.int32, (n_own, sel), 0)
    iota_lo = lax.broadcasted_iota(jnp.int32, (128, sel), 0)

    def body(grp, carry):
        base = pl.multiple_of(grp * 8, 8)
        pick = pick_ref[pl.ds(base, 8), :]
        hi = pick >> 7
        lo = pick & 127
        parts = [piece.astype(F32) for piece in split3(gate_ref[pl.ds(base, 8), :])]
        for j in range(8):
            mask = iota_own == hi[j:j + 1, :]
            left = jnp.concatenate([jnp.where(mask, piece[j:j + 1, :], 0.0).astype(BF16) for piece in parts], axis=0)
            right = jnp.where(iota_lo == lo[j:j + 1, :], 1.0, 0.0).astype(BF16)
            res = dot_nt(left, right)
            tile_ref[j * n_own:(j + 1) * n_own, :] = res[:n_own] + res[n_own:2 * n_own] + res[2 * n_own:]
        for o in range(n_own):
            out_ref[pl.ds(base, 8), o * 128:(o + 1) * 128] = tile_ref[pl.ds(o, 8, stride=n_own), :]
        return carry

    lax.fori_loop(0, pick_ref.shape[0] // 8, body, 0)


def gate_matrix(pick_rel, gate, n_own):
    tok, sel = pick_rel.shape
    blk = max(8, tok // 4)
    return pl.pallas_call(
        functools.partial(gate_kernel, n_own),
        grid=(tok // blk,),
        in_specs=[pl.BlockSpec((blk, sel), lambda i: (i, 0)), pl.BlockSpec((blk, sel), lambda i: (i, 0))],
        out_specs=pl.BlockSpec((blk, n_own * 128), lambda i: (i, 0)),
        out_shape=jax.ShapeDtypeStruct((tok, n_own * 128), F32),
        scratch_shapes=[pltpu.VMEM((8 * n_own, 128), F32)],
        compiler_params=pltpu.CompilerParams(vmem_limit_bytes=VMEM_LIMIT),
        cost_estimate=pl.CostEstimate(flops=2 * tok * 256 * 256 * 192, bytes_accessed=tok * n_own * 512, transcendentals=0),
        name="gate_matrix",
    )(pick_rel, gate)


def select_rows(tab_ref, idsb_ref, sel_ref):
    n_rows = tab_ref.shape[0] // OWN_STEP
    iota = lax.broadcasted_iota(jnp.int32, (128, 128), 1)
    my_x = lax.axis_index('table') % 4
    for j in range(OWN_STEP):
        ids = idsb_ref[j * 128:(j + 1) * 128, :]
        hot = jnp.concatenate([jnp.where(ids == iota + 128 * h, 1.0, 0.0).astype(BF16) for h in range(n_rows // 128)], axis=1)
        start = pl.multiple_of(xor_field(j, my_x) * n_rows, n_rows)
        sel_ref[j * 128:(j + 1) * 128, :] = dot_nn(hot, tab_ref[pl.ds(start, n_rows), :]).astype(BF16)


def place_rows(blk, grad_t, ids_ref, keep_ref, send_ref):
    iota = lax.broadcasted_iota(jnp.int32, (256, 128), 0)
    grad_b = grad_t.astype(BF16)
    for j in range(OWN_STEP):
        hot = jnp.where(iota == ids_ref[pl.ds(blk * OWN_STEP + j, 1), :], 1.0, 0.0).astype(BF16)
        rows = dot_nt(hot, grad_b[:, j * 128:(j + 1) * 128]).astype(BF16)
        keep_ref[j * 128:(j + 1) * 128, :] = rows[:128]
        send_ref[j * 128:(j + 1) * 128, :] = rows[128:]


def first_kernel(tok_ref, dyt_ref, tab_ref, idsb_ref, ids_ref, gate_ref, w_ref, slope_ref, sel_ref, keep_ref, send_ref):
    select_rows(tab_ref, idsb_ref, sel_ref)
    pre = dot_nt(tok_ref[...], sel_ref[...])
    gate = gate_ref[...]
    cdf = 0.5 * (1.0 + lax.erf(pre * 0.7071067811865476))
    pdf = jnp.exp(-0.5 * pre * pre) * 0.3989422804014327
    live = gate != 0.0
    w = jnp.where(live, gate * (pre * cdf), 0.0)
    w_ref[...] = w
    slope_ref[...] = jnp.where(live, gate * (cdf + pre * pdf), 0.0)
    one, two, three = split3(w)
    dyt = dyt_ref[...]
    grad_t = dot_nn(dyt, one) + dot_nn(dyt, two) + dot_nn(dyt, three)
    place_rows(pl.program_id(0), grad_t, ids_ref, keep_ref, send_ref)


def first_pass(tok, dyt, table, idsb, ids_flip, gate):
    n_tok, width = tok.shape
    n_list = gate.shape[1]
    cols = OWN_STEP * 128
    steps = n_list // cols
    trows = table.shape[0] // steps
    row_blk = pl.BlockSpec((cols, width), lambda i: (i, 0))
    mat_blk = pl.BlockSpec((n_tok, cols), lambda i: (0, i))
    return pl.pallas_call(
        first_kernel,
        grid=(steps,),
        in_specs=[
            pl.BlockSpec((n_tok, width), lambda i: (0, 0)),
            pl.BlockSpec((width, n_tok), lambda i: (0, 0)),
            pl.BlockSpec((trows, width), lambda i: (table_block(i), 0)),
            pl.BlockSpec((cols, 128), lambda i: (i, 0)),
            pl.BlockSpec(ids_flip.shape, lambda i: (0, 0)),
            mat_blk,
        ],
        out_specs=[mat_blk, mat_blk, row_blk, row_blk, row_blk],
        out_shape=[
            jax.ShapeDtypeStruct((n_tok, n_list), F32),
            jax.ShapeDtypeStruct((n_tok, n_list), F32),
            jax.ShapeDtypeStruct((n_list, width), BF16),
            jax.ShapeDtypeStruct((n_list, width), BF16),
            jax.ShapeDtypeStruct((n_list, width), BF16),
        ],
        compiler_params=pltpu.CompilerParams(vmem_limit_bytes=VMEM_LIMIT),
        cost_estimate=pl.CostEstimate(flops=11 * n_tok * n_list * width, bytes_accessed=n_list * (width * 10 + n_tok * 12), transcendentals=0),
        name="first_pass",
    )(tok, dyt, table, idsb, ids_flip, gate)


class Reducer:
    N_COPIES = 9

    @staticmethod
    def scratch(width):
        shapes = []
        for k in range(3):
            rows = ROW_CUTS[k + 1] - ROW_CUTS[k]
            lead = [(2, SIDE, SIDE), (2, SIDE, SIDE), (SIDE, SIDE), (2, SIDE), (SIDE,), (2,), (1,)]
            shapes += [pltpu.VMEM(dims + (rows, width), BF16) for dims in lead]
        return shapes + [pltpu.SemaphoreType.DMA((27,)), pltpu.SemaphoreType.DMA((27,)), pltpu.SemaphoreType.DMA((6,))]

    def __init__(self, src, out, scratch):
        self.src, self.out = src, out
        self.bufs = [scratch[7 * k:7 * k + 7] for k in range(3)]
        self.send_sem, self.recv_sem, self.load_sem = scratch[21:]
        core = lax.axis_index('data')
        self.core = core
        self.near, self.far = 1 + 2 * core, 3 - 2 * core

    def partner(self, axis, first):
        me = lax.axis_index('table')
        stride = SIDE ** (2 - axis)
        pos = (me // stride) % SIDE
        even, odd = pos + 1 - 2 * (pos % 2), 3 - pos
        new = even + self.core * (odd - even) if first else odd + self.core * (even - odd)
        return me + (new - pos) * stride

    def remote(self, k, num, src, dst, axis, first):
        at = k * self.N_COPIES + num
        return pltpu.make_async_remote_copy(src_ref=src, dst_ref=dst, send_sem=self.send_sem.at[at], recv_sem=self.recv_sem.at[at], device_id={'table': self.partner(axis, first)}, device_id_type=pl.DeviceIdType.MESH)

    def slab(self, k, slot):
        idx = [slice(None)] * 3
        idx[AXIS_ORDERS[k][0]] = slot
        return self.src.at[idx[0], idx[1], idx[2], pl.ds(ROW_CUTS[k], ROW_CUTS[k + 1] - ROW_CUTS[k])]

    def order(self, k, b, c):
        return (b, c) if AXIS_ORDERS[k][1] < AXIS_ORDERS[k][2] else (c, b)

    def loads(self):
        return [pltpu.make_async_copy(self.slab(k, slot), self.bufs[k][0].at[j], self.load_sem.at[2 * k + j]) for k in range(3) for j, slot in enumerate((0, self.far))]

    def copies(self, stage):
        out = []
        for k in range(3):
            a, b, c = AXIS_ORDERS[k]
            held, got1, got2, got3, got4, got5, got6 = self.bufs[k]
            if stage == 1:
                out += [self.remote(k, j, self.slab(k, slot), got1.at[j], a, True) for j, slot in enumerate((self.near, 2))]
            elif stage == 2:
                out.append(self.remote(k, 2, held.at[1], got2, a, False))
            elif stage == 3:
                out += [self.remote(k, 3 + j, self.row_of(k, held, slot), got3.at[j], b, True) for j, slot in enumerate((self.near, 2))]
            elif stage == 4:
                out.append(self.remote(k, 5, self.row_of(k, held, self.far), got4, b, False))
            elif stage == 5:
                out += [self.remote(k, 6 + j, held.at[(0,) + self.order(k, 0, slot)], got5.at[j], c, True) for j, slot in enumerate((self.near, 2))]
            else:
                out.append(self.remote(k, 8, held.at[(0,) + self.order(k, 0, self.far)], got6.at[0], c, False))
        return out

    def row_of(self, k, held, slot):
        p, q = self.order(k, slot, slice(None))
        return held.at[0, p, q]

    def terms(self, k, b, c, depth):
        held, got1, got2, got3, got4, got5, got6 = self.bufs[k]
        p, q = self.order(k, b, c)
        arrs = [held[0, p, q], got1[0, p, q], got2[p, q]]
        return p, q, arrs

    def total(self, arrs):
        return functools.reduce(jnp.add, [arr.astype(F32) for arr in arrs])

    def add(self, stage):
        for k in range(3):
            held, got1, got2, got3, got4, got5, got6 = self.bufs[k]
            if stage == 2:
                def body(i, carry):
                    p, q = i // SIDE, i % SIDE
                    held[1, p, q] = self.total([held[1, p, q], got1[1, p, q]]).astype(BF16)
                    return carry
                lax.fori_loop(0, SIDE * SIDE, body, 0)
            elif stage == 3:
                def body(i, carry):
                    j = i // SIDE
                    p, q, arrs = self.terms(k, self.near + j * (2 - self.near), i % SIDE, 3)
                    held[0, p, q] = self.total(arrs).astype(BF16)
                    return carry
                lax.fori_loop(0, 2 * SIDE, body, 0)
            elif stage == 4:
                def body(c, carry):
                    p, q, arrs = self.terms(k, self.far, c, 4)
                    held[0, p, q] = self.total(arrs + [got3[1, c]]).astype(BF16)
                    return carry
                lax.fori_loop(0, SIDE, body, 0)
            elif stage == 5:
                for slot in (self.near, 2):
                    p, q, arrs = self.terms(k, 0, slot, 5)
                    held[0, p, q] = self.total(arrs + [got3[0, slot], got4[slot]]).astype(BF16)
            elif stage == 6:
                p, q, arrs = self.terms(k, 0, self.far, 6)
                held[0, p, q] = self.total(arrs + [got3[0, self.far], got4[self.far], got5[1]]).astype(BF16)
            else:
                p, q, arrs = self.terms(k, 0, 0, 7)
                self.out[ROW_CUTS[k]:ROW_CUTS[k + 1], :] = self.total(arrs + [got3[0, 0], got4[0], got5[0], got6[0]]).astype(self.out.dtype)

    def run(self, stage):
        if stage == 1:
            for copy in self.loads():
                copy.start()
        else:
            if stage == 2:
                for copy in self.loads():
                    copy.wait()
            for copy in self.copies(stage - 1):
                copy.wait_recv()
            self.add(stage)
        if stage < 7:
            for copy in self.copies(stage):
                copy.start()
        else:
            for done in range(1, 7):
                for copy in self.copies(done):
                    copy.wait_send()


def run_stages(reducer, step, last, marks):
    for stage, mark in marks:
        if last is None and mark is not None:
            pl.when(step == mark)(functools.partial(reducer.run, stage))
    if last is not None:
        @pl.when(step == last)
        def _():
            for stage, mark in marks:
                if mark is None:
                    reducer.run(stage)


SECOND_MARKS = ((1, 0), (2, 9), (3, 14), (4, None), (5, None), (6, None), (7, None))
OUT_MARKS = ((1, 0), (2, None), (3, None), (4, None), (5, None), (6, None), (7, None))


def second_kernel(dy_ref, tokt_ref, tab_ref, idsb_ref, ids_ref, slope_ref, part_ref, c_ref, sel_ref, keep_ref, send_ref, red_ref, *scratch):
    step = pl.program_id(0)
    reducer = Reducer(part_ref, red_ref, scratch)
    run_stages(reducer, step, None, SECOND_MARKS)
    select_rows(tab_ref, idsb_ref, sel_ref)
    back = dot_nt(dy_ref[...], sel_ref[...])
    slope = slope_ref[...]
    c = jnp.where(slope != 0.0, slope * back, 0.0)
    c_ref[...] = c
    one, two, three = split3(c)
    tokt = tokt_ref[...]
    grad_t = dot_nn(tokt, one) + dot_nn(tokt, two) + dot_nn(tokt, three)
    place_rows(step, grad_t, ids_ref, keep_ref, send_ref)
    run_stages(reducer, step, pl.num_programs(0) - 1, SECOND_MARKS)


def second_pass(dy, tokt, table, idsb, ids_flip, slope, part):
    n_tok, width = dy.shape
    n_list = slope.shape[1]
    cols = OWN_STEP * 128
    steps = n_list // cols
    trows = table.shape[0] // steps
    row_blk = pl.BlockSpec((cols, width), lambda i: (i, 0))
    mat_blk = pl.BlockSpec((n_tok, cols), lambda i: (0, i))
    return pl.pallas_call(
        second_kernel,
        grid=(steps,),
        in_specs=[
            pl.BlockSpec((n_tok, width), lambda i: (0, 0)),
            pl.BlockSpec((width, n_tok), lambda i: (0, 0)),
            pl.BlockSpec((trows, width), lambda i: (table_block(i), 0)),
            pl.BlockSpec((cols, 128), lambda i: (i, 0)),
            pl.BlockSpec(ids_flip.shape, lambda i: (0, 0)),
            mat_blk,
            pl.BlockSpec(memory_space=pl.ANY),
        ],
        out_specs=[mat_blk, row_blk, row_blk, row_blk, pl.BlockSpec((128, width), lambda i: (0, 0))],
        out_shape=[
            jax.ShapeDtypeStruct((n_tok, n_list), F32),
            jax.ShapeDtypeStruct((n_list, width), BF16),
            jax.ShapeDtypeStruct((n_list, width), BF16),
            jax.ShapeDtypeStruct((n_list, width), BF16),
            jax.ShapeDtypeStruct((128, width), BF16),
        ],
        scratch_shapes=Reducer.scratch(width),
        compiler_params=pltpu.CompilerParams(vmem_limit_bytes=VMEM_LIMIT, has_side_effects=True),
        cost_estimate=pl.CostEstimate(flops=11 * n_tok * n_list * width, bytes_accessed=n_list * (width * 10 + n_tok * 8), transcendentals=0),
        name="second_pass",
    )(dy, tokt, table, idsb, ids_flip, slope, part)


def out_step(mat_ref, row_ref, out_ref, acc_ref):
    step = pl.program_id(0)
    one, two, three = split3(mat_ref[...])
    rows = row_ref[...]
    part = dot_nn(one, rows) + dot_nn(two, rows) + dot_nn(three, rows)

    @pl.when(step == 0)
    def _():
        acc_ref[...] = part

    @pl.when(step > 0)
    def _():
        acc_ref[...] += part

    @pl.when(step == pl.num_programs(0) - 1)
    def _():
        out_ref[...] = acc_ref[...].astype(out_ref.dtype)


def out_reduce_step(mat_ref, row_ref, part_ref, out_ref, red_ref, acc_ref, *scratch):
    step = pl.program_id(0)
    reducer = Reducer(part_ref, red_ref, scratch)
    run_stages(reducer, step, None, OUT_MARKS)
    out_step(mat_ref, row_ref, out_ref, acc_ref)
    run_stages(reducer, step, pl.num_programs(0) - 1, OUT_MARKS)


def out_pass(mat, rows, part=None):
    n_tok, n_list = mat.shape
    width = rows.shape[1]
    cols = 1024
    extra = part is not None
    return pl.pallas_call(
        out_reduce_step if extra else out_step,
        grid=(n_list // cols,),
        in_specs=[pl.BlockSpec((n_tok, cols), lambda i: (0, i)), pl.BlockSpec((cols, width), lambda i: (i, 0))] + [pl.BlockSpec(memory_space=pl.ANY)] * extra,
        out_specs=[pl.BlockSpec((n_tok, width), lambda i: (0, 0))] + [pl.BlockSpec((128, width), lambda i: (0, 0))] * extra,
        out_shape=[jax.ShapeDtypeStruct((n_tok, width), BF16)] + [jax.ShapeDtypeStruct((128, width), BF16)] * extra,
        scratch_shapes=[pltpu.VMEM((n_tok, width), F32)] + (Reducer.scratch(width) if extra else []),
        compiler_params=pltpu.CompilerParams(vmem_limit_bytes=VMEM_LIMIT, has_side_effects=extra),
        cost_estimate=pl.CostEstimate(flops=6 * n_tok * n_list * width, bytes_accessed=n_list * (width * 2 + n_tok * 4), transcendentals=0),
        name="out_reduce" if extra else "out_pass",
    )(mat, rows, *([part] if extra else []))


def solution(mesh):
    table_n = mesh.shape['table']
    tok_spec = P(('replica', 'data', 'table'))
    row_spec = P(('replica', 'table'))

    def device_step(tok, dy, u_loc, v_loc, wanted, pick, gate):
        n_local, width = u_loc.shape
        half = n_local // 2
        n_tok = tok.shape[0]
        core = lax.axis_index('data')
        me = lax.axis_index('table')
        own_rows = lambda arr: lax.dynamic_slice_in_dim(arr, core * half, half, 0)
        full_u = lax.all_gather(own_rows(u_loc), ('table', 'data'), axis=0, tiled=True)
        full_v = lax.all_gather(own_rows(v_loc), ('table', 'data'), axis=0, tiled=True)

        owners = jnp.arange(table_n, dtype=jnp.int32) ^ me
        ids = jnp.take(wanted.reshape(table_n, -1), owners, axis=0, mode='clip') - owners[:, None] * n_local
        ids_flip = ids ^ (core * half)
        idsb = jnp.broadcast_to(ids.reshape(-1, 1), (ids.size, 128))
        pick_rel = pick.reshape(n_tok, -1) ^ (me << 7)
        gates = gate_matrix(pick_rel, gate.reshape(n_tok, -1), table_n)

        swap = [(i, (i + table_n) % (2 * table_n)) for i in range(2 * table_n)]
        cube = (SIDE, SIDE, SIDE, half, width)

        def pair_sum(keep, send):
            got = lax.ppermute(send, ('data', 'table'), swap)
            return (keep.astype(F32) + got.astype(F32)).astype(BF16).reshape(cube)

        both_cores = lambda rows: lax.all_gather(rows, 'data', axis=0, tiled=True)
        w, slope, u_sel, keep_v, send_v = first_pass(tok, dy.T, full_u, idsb, ids_flip, gates)
        c, v_sel, keep_u, send_u, red_v = second_pass(dy, tok.T, full_v, idsb, ids_flip, slope, pair_sum(keep_v, send_v))
        grad_v = both_cores(red_v)
        part_u = pair_sum(keep_u, send_u)
        y, = out_pass(w, v_sel)
        part_u, y = lax.optimization_barrier((part_u, y))
        dx, red_u = out_pass(c, u_sel, part_u)
        grad_u = both_cores(red_u)
        return y, dx, grad_u, grad_v

    return jax.shard_map(device_step, mesh=mesh, in_specs=(tok_spec, tok_spec, row_spec, row_spec, tok_spec, tok_spec, tok_spec), out_specs=(tok_spec, tok_spec, row_spec, row_spec), check_vma=False)
```

```python
import functools
import jax
import jax.numpy as jnp
from jax import lax
from jax.experimental import pallas as pl
from jax.experimental.pallas import tpu as pltpu
from jax.sharding import PartitionSpec as P

F32 = jnp.float32
BF16 = jnp.bfloat16
SIDE = 4
OWN_STEP = 4
VMEM_LIMIT = 60 * 1024 * 1024
ROW_CUTS = (0, 48, 96, 128)
AXIS_ORDERS = ((2, 1, 0), (1, 0, 2), (0, 2, 1))


def split3(val):
    one = val.astype(BF16)
    rest = val - one.astype(F32)
    two = rest.astype(BF16)
    rest = rest - two.astype(F32)
    return one, two, rest.astype(BF16)


def dot_nn(lhs, rhs):
    return lax.dot_general(lhs, rhs, (((1,), (0,)), ((), ())), preferred_element_type=F32)


def dot_nt(lhs, rhs):
    return lax.dot_general(lhs, rhs, (((1,), (1,)), ((), ())), preferred_element_type=F32)


def xor_field(val, other):
    return (val // 2 + other // 2) % 2 * 2 + (val % 2 + other % 2) % 2


def table_block(step):
    me = lax.axis_index('table')
    return xor_field(step // 4, me // 16) * 4 + xor_field(step % 4, (me // 4) % 4)


def gate_kernel(n_own, pick_ref, gate_ref, out_ref, tile_ref):
    sel = pick_ref.shape[1]
    iota_own = lax.broadcasted_iota(jnp.int32, (n_own, sel), 0)
    iota_lo = lax.broadcasted_iota(jnp.int32, (128, sel), 0)

    def body(grp, carry):
        base = pl.multiple_of(grp * 8, 8)
        pick = pick_ref[pl.ds(base, 8), :]
        hi = pick >> 7
        lo = pick & 127
        parts = [piece.astype(F32) for piece in split3(gate_ref[pl.ds(base, 8), :])]
        for j in range(8):
            mask = iota_own == hi[j:j + 1, :]
            left = jnp.concatenate([jnp.where(mask, piece[j:j + 1, :], 0.0).astype(BF16) for piece in parts], axis=0)
            right = jnp.where(iota_lo == lo[j:j + 1, :], 1.0, 0.0).astype(BF16)
            res = dot_nt(left, right)
            tile_ref[j * n_own:(j + 1) * n_own, :] = res[:n_own] + res[n_own:2 * n_own] + res[2 * n_own:]
        for o in range(n_own):
            out_ref[pl.ds(base, 8), o * 128:(o + 1) * 128] = tile_ref[pl.ds(o, 8, stride=n_own), :]
        return carry

    lax.fori_loop(0, pick_ref.shape[0] // 8, body, 0)


def gate_matrix(pick_rel, gate, n_own):
    tok, sel = pick_rel.shape
    blk = max(8, tok // 4)
    return pl.pallas_call(
        functools.partial(gate_kernel, n_own),
        grid=(tok // blk,),
        in_specs=[pl.BlockSpec((blk, sel), lambda i: (i, 0)), pl.BlockSpec((blk, sel), lambda i: (i, 0))],
        out_specs=pl.BlockSpec((blk, n_own * 128), lambda i: (i, 0)),
        out_shape=jax.ShapeDtypeStruct((tok, n_own * 128), F32),
        scratch_shapes=[pltpu.VMEM((8 * n_own, 128), F32)],
        compiler_params=pltpu.CompilerParams(vmem_limit_bytes=VMEM_LIMIT),
        cost_estimate=pl.CostEstimate(flops=2 * tok * 256 * 256 * 192, bytes_accessed=tok * n_own * 512, transcendentals=0),
        name="gate_matrix",
    )(pick_rel, gate)


def select_rows(tab_ref, idsb_ref, sel_ref):
    n_rows = tab_ref.shape[0] // OWN_STEP
    iota = lax.broadcasted_iota(jnp.int32, (128, 128), 1)
    my_x = lax.axis_index('table') % 4
    for j in range(OWN_STEP):
        ids = idsb_ref[j * 128:(j + 1) * 128, :]
        hot = jnp.concatenate([jnp.where(ids == iota + 128 * h, 1.0, 0.0).astype(BF16) for h in range(n_rows // 128)], axis=1)
        start = pl.multiple_of(xor_field(j, my_x) * n_rows, n_rows)
        sel_ref[j * 128:(j + 1) * 128, :] = dot_nn(hot, tab_ref[pl.ds(start, n_rows), :]).astype(BF16)


def place_rows(blk, grad_t, ids_ref, slot, keep_ref, send_ref):
    iota = lax.broadcasted_iota(jnp.int32, (256, 128), 0)
    grad_b = grad_t.astype(BF16)
    for j in range(OWN_STEP):
        hot = jnp.where(iota == ids_ref[pl.ds(blk * OWN_STEP + j, 1), :], 1.0, 0.0).astype(BF16)
        rows = dot_nt(hot, grad_b[:, j * 128:(j + 1) * 128]).astype(BF16)
        keep_ref[slot, j] = rows[:128]
        send_ref[slot, j] = rows[128:]


LAG = 3


class Exchanger:
    @staticmethod
    def scratch(width):
        blk = (2, OWN_STEP, 128, width)
        dma = pltpu.SemaphoreType.DMA
        return [pltpu.VMEM(blk, BF16)] * 4 + [dma((2,)), dma((2,)), dma((8,)), dma((6,))]

    @staticmethod
    def out_shapes(width):
        rows = [ROW_CUTS[k + 1] - ROW_CUTS[k] for k in range(3)]
        cube = jax.ShapeDtypeStruct((SIDE, SIDE, SIDE, 128, width), BF16)
        return [cube] + [jax.ShapeDtypeStruct((2, SIDE, SIDE, n, width), BF16) for n in rows]

    @staticmethod
    def out_specs(width, blocks):
        def place(i):
            blk = jnp.clip(i - 2, 0, blocks - 1)
            return blk // SIDE, blk % SIDE, 0, 0, 0
        return [pl.BlockSpec((1, 1, SIDE, 128, width), place)] + [pl.BlockSpec(memory_space=pl.ANY)] * 3

    def __init__(self, step, blocks, outs, scratch):
        self.step, self.blocks = step, blocks
        self.part_ref, self.first = outs[0], outs[1:]
        self.keep, self.send, self.got, self.sum = scratch[:4]
        self.pair_send, self.pair_recv, self.out_send, self.out_recv = scratch[4:]
        self.ring = Ring()

    def pair_copy(self, slot):
        other = 1 - lax.axis_index('data')
        return pltpu.make_async_remote_copy(src_ref=self.send.at[slot], dst_ref=self.got.at[slot], send_sem=self.pair_send.at[slot], recv_sem=self.pair_recv.at[slot], device_id={'data': other}, device_id_type=pl.DeviceIdType.MESH)

    def first_copies(self, blk):
        slot = blk % 2
        spots = (blk // SIDE, blk % SIDE)
        out = []
        near = self.ring.near

        def copy(k, num, src, dst, way):
            return pltpu.make_async_remote_copy(src_ref=src, dst_ref=dst, send_sem=self.out_send.at[4 * slot + num], recv_sem=self.out_recv.at[2 * k + way], device_id={'table': self.ring.partner(AXIS_ORDERS[k][0], True)}, device_id_type=pl.DeviceIdType.MESH)

        for k in range(3):
            axis = AXIS_ORDERS[k][0]
            rows = pl.ds(ROW_CUTS[k], ROW_CUTS[k + 1] - ROW_CUTS[k])
            if axis == 2:
                for way, x in enumerate((near, 2)):
                    out.append((None, copy(k, way, self.sum.at[slot, x, rows], self.first[k].at[way, spots[0], spots[1]], way)))
            else:
                for way, mark in enumerate((near, 2)):
                    out.append((spots[axis] == mark, copy(k, 3 - axis, self.sum.at[slot, :, rows], self.first[k].at[way, spots[1 - axis]], way)))
        return out

    def on_first(self, blk, act):
        for cond, copy in self.first_copies(blk):
            if cond is None:
                act(copy)
            else:
                pl.when(cond)(functools.partial(act, copy))

    def before(self):
        step, blocks = self.step, self.blocks

        @pl.when((step >= 4) & (step - 4 < blocks))
        def _():
            self.on_first(step - 4, lambda copy: copy.wait_send())

        @pl.when((step >= 3) & (step - 3 < blocks))
        def _():
            self.on_first(step - 3, lambda copy: copy.start())

        @pl.when((step >= 2) & (step - 2 < blocks))
        def _():
            slot = step % 2
            copy = self.pair_copy(slot)
            copy.wait_recv()
            for j in range(OWN_STEP):
                rows = (self.keep[slot, j].astype(F32) + self.got[slot, j].astype(F32)).astype(BF16)
                self.sum[slot, j] = rows
                self.part_ref[0, 0, j] = rows
            copy.wait_send()

        @pl.when((step >= 1) & (step - 1 < blocks))
        def _():
            self.pair_copy((step - 1) % 2).start()

    def after(self):
        @pl.when(self.step == self.blocks + LAG - 1)
        def _():
            self.on_first(self.blocks - 1, lambda copy: copy.wait_send())
            for k in range(3):
                for way in range(2):
                    dst = self.first[k].at[way]
                    pltpu.make_async_copy(dst, dst, self.out_recv.at[2 * k + way]).wait()


class Ring:
    def __init__(self):
        self.core = lax.axis_index('data')
        self.near, self.far = 1 + 2 * self.core, 3 - 2 * self.core

    def partner(self, axis, first):
        me = lax.axis_index('table')
        stride = SIDE ** (2 - axis)
        pos = (me // stride) % SIDE
        even, odd = pos + 1 - 2 * (pos % 2), 3 - pos
        new = even + self.core * (odd - even) if first else odd + self.core * (even - odd)
        return me + (new - pos) * stride


def first_kernel(tok_ref, dyt_ref, tab_ref, idsb_ref, ids_ref, gate_ref, w_ref, slope_ref, sel_ref, *rest):
    step = pl.program_id(0)
    blocks = pl.num_programs(0) - LAG
    swap = Exchanger(step, blocks, rest[:4], rest[4:])
    swap.before()

    @pl.when(step < blocks)
    def _():
        select_rows(tab_ref, idsb_ref, sel_ref)
        pre = dot_nt(tok_ref[...], sel_ref[...])
        gate = gate_ref[...]
        cdf = 0.5 * (1.0 + lax.erf(pre * 0.7071067811865476))
        pdf = jnp.exp(-0.5 * pre * pre) * 0.3989422804014327
        live = gate != 0.0
        w = jnp.where(live, gate * (pre * cdf), 0.0)
        w_ref[...] = w
        slope_ref[...] = jnp.where(live, gate * (cdf + pre * pdf), 0.0)
        one, two, three = split3(w)
        dyt = dyt_ref[...]
        grad_t = dot_nn(dyt, one) + dot_nn(dyt, two) + dot_nn(dyt, three)
        place_rows(step, grad_t, ids_ref, step % 2, swap.keep, swap.send)

    swap.after()


def first_pass(tok, dyt, table, idsb, ids_flip, gate):
    n_tok, width = tok.shape
    n_list = gate.shape[1]
    cols = OWN_STEP * 128
    steps = n_list // cols
    trows = table.shape[0] // steps
    at = lambda i: jnp.minimum(i, steps - 1)
    row_blk = pl.BlockSpec((cols, width), lambda i: (at(i), 0))
    mat_blk = pl.BlockSpec((n_tok, cols), lambda i: (0, at(i)))
    return pl.pallas_call(
        first_kernel,
        grid=(steps + LAG,),
        in_specs=[
            pl.BlockSpec((n_tok, width), lambda i: (0, 0)),
            pl.BlockSpec((width, n_tok), lambda i: (0, 0)),
            pl.BlockSpec((trows, width), lambda i: (table_block(at(i)), 0)),
            pl.BlockSpec((cols, 128), lambda i: (at(i), 0)),
            pl.BlockSpec(ids_flip.shape, lambda i: (0, 0)),
            mat_blk,
        ],
        out_specs=[mat_blk, mat_blk, row_blk] + Exchanger.out_specs(width, steps),
        out_shape=[
            jax.ShapeDtypeStruct((n_tok, n_list), F32),
            jax.ShapeDtypeStruct((n_tok, n_list), F32),
            jax.ShapeDtypeStruct((n_list, width), BF16),
        ] + Exchanger.out_shapes(width),
        scratch_shapes=Exchanger.scratch(width),
        compiler_params=pltpu.CompilerParams(vmem_limit_bytes=VMEM_LIMIT, has_side_effects=True),
        cost_estimate=pl.CostEstimate(flops=11 * n_tok * n_list * width, bytes_accessed=n_list * (width * 10 + n_tok * 12), transcendentals=0),
        name="first_pass",
    )(tok, dyt, table, idsb, ids_flip, gate)


class Reducer(Ring):
    N_COPIES = 9

    @staticmethod
    def scratch(width):
        shapes = []
        for k in range(3):
            rows = ROW_CUTS[k + 1] - ROW_CUTS[k]
            lead = [(2, SIDE, SIDE), (2, SIDE, SIDE), (SIDE, SIDE), (2, SIDE), (SIDE,), (2,), (1,)]
            shapes += [pltpu.VMEM(dims + (rows, width), BF16) for dims in lead]
        return shapes + [pltpu.SemaphoreType.DMA((27,)), pltpu.SemaphoreType.DMA((27,)), pltpu.SemaphoreType.DMA((12,))]

    def __init__(self, src, first, out, scratch):
        super().__init__()
        self.src, self.first, self.out = src, first, out
        self.bufs = [scratch[7 * k:7 * k + 7] for k in range(3)]
        self.send_sem, self.recv_sem, self.load_sem = scratch[21:]

    def remote(self, k, num, src, dst, axis, first):
        at = k * self.N_COPIES + num
        return pltpu.make_async_remote_copy(src_ref=src, dst_ref=dst, send_sem=self.send_sem.at[at], recv_sem=self.recv_sem.at[at], device_id={'table': self.partner(axis, first)}, device_id_type=pl.DeviceIdType.MESH)

    def slab(self, k, slot):
        idx = [slice(None)] * 3
        idx[AXIS_ORDERS[k][0]] = slot
        return self.src.at[idx[0], idx[1], idx[2], pl.ds(ROW_CUTS[k], ROW_CUTS[k + 1] - ROW_CUTS[k])]

    def order(self, k, b, c):
        return (b, c) if AXIS_ORDERS[k][1] < AXIS_ORDERS[k][2] else (c, b)

    def loads(self):
        own = [pltpu.make_async_copy(self.slab(k, slot), self.bufs[k][0].at[j], self.load_sem.at[2 * k + j]) for j, slot in ((1, self.far), (0, 0)) for k in range(3)]
        come = [pltpu.make_async_copy(self.first[k].at[j], self.bufs[k][1].at[j], self.load_sem.at[6 + 2 * k + j]) for j in (1, 0) for k in range(3)]
        return [copy for j in range(2) for copy in own[3 * j:3 * j + 3] + come[3 * j:3 * j + 3]]

    def copies(self, stage):
        out = []
        for k in range(3):
            a, b, c = AXIS_ORDERS[k]
            held, got1, got2, got3, got4, got5, got6 = self.bufs[k]
            if stage == 2:
                out.append(self.remote(k, 2, held.at[1], got2, a, False))
            elif stage == 3:
                out += [self.remote(k, 3 + j, self.row_of(k, held, slot), got3.at[j], b, True) for j, slot in enumerate((self.near, 2))]
            elif stage == 4:
                out.append(self.remote(k, 5, self.row_of(k, held, self.far), got4, b, False))
            elif stage == 5:
                out += [self.remote(k, 6 + j, held.at[(0,) + self.order(k, 0, slot)], got5.at[j], c, True) for j, slot in enumerate((self.near, 2))]
            else:
                out.append(self.remote(k, 8, held.at[(0,) + self.order(k, 0, self.far)], got6.at[0], c, False))
        return out

    def row_of(self, k, held, slot):
        p, q = self.order(k, slot, slice(None))
        return held.at[0, p, q]

    def terms(self, k, b, c, depth):
        held, got1, got2, got3, got4, got5, got6 = self.bufs[k]
        p, q = self.order(k, b, c)
        arrs = [held[0, p, q], got1[0, p, q], got2[p, q]]
        return p, q, arrs

    def total(self, arrs):
        return functools.reduce(jnp.add, [arr.astype(F32) for arr in arrs])

    def add(self, stage):
        for k in range(3):
            held, got1, got2, got3, got4, got5, got6 = self.bufs[k]
            if stage == 2:
                def body(i, carry):
                    p, q = i // SIDE, i % SIDE
                    held[1, p, q] = self.total([held[1, p, q], got1[1, p, q]]).astype(BF16)
                    return carry
                lax.fori_loop(0, SIDE * SIDE, body, 0)
            elif stage == 3:
                def body(i, carry):
                    j = i // SIDE
                    p, q, arrs = self.terms(k, self.near + j * (2 - self.near), i % SIDE, 3)
                    held[0, p, q] = self.total(arrs).astype(BF16)
                    return carry
                lax.fori_loop(0, 2 * SIDE, body, 0)
            elif stage == 4:
                def body(c, carry):
                    p, q, arrs = self.terms(k, self.far, c, 4)
                    held[0, p, q] = self.total(arrs + [got3[1, c]]).astype(BF16)
                    return carry
                lax.fori_loop(0, SIDE, body, 0)
            elif stage == 5:
                for slot in (self.near, 2):
                    p, q, arrs = self.terms(k, 0, slot, 5)
                    held[0, p, q] = self.total(arrs + [got3[0, slot], got4[slot]]).astype(BF16)
            elif stage == 6:
                p, q, arrs = self.terms(k, 0, self.far, 6)
                held[0, p, q] = self.total(arrs + [got3[0, self.far], got4[self.far], got5[1]]).astype(BF16)
            else:
                p, q, arrs = self.terms(k, 0, 0, 7)
                self.out[ROW_CUTS[k]:ROW_CUTS[k + 1], :] = self.total(arrs + [got3[0, 0], got4[0], got5[0], got6[0]]).astype(self.out.dtype)

    def run(self, stage):
        if stage == 1:
            for copy in self.loads():
                copy.start()
            return
        if stage == 2:
            for copy in self.loads():
                copy.wait()
        else:
            for copy in self.copies(stage - 1):
                copy.wait_recv()
        self.add(stage)
        if stage < 7:
            for copy in self.copies(stage):
                copy.start()
        else:
            for done in range(2, 7):
                for copy in self.copies(done):
                    copy.wait_send()


def run_stages(reducer, step, last, marks):
    for stage, mark in marks:
        if last is None and mark is not None:
            pl.when(step == mark)(functools.partial(reducer.run, stage))
    if last is not None:
        @pl.when(step == last)
        def _():
            for stage, mark in marks:
                if mark is None:
                    reducer.run(stage)


SECOND_MARKS = ((1, 0), (2, 2), (3, 8), (4, 12), (5, 14), (6, 16), (7, None))
OUT_MARKS = ((1, 0), (2, 2), (3, 8), (4, 11), (5, 13), (6, 15), (7, None))


def second_kernel(dy_ref, tokt_ref, tab_ref, idsb_ref, ids_ref, slope_ref, part_ref, f0_ref, f1_ref, f2_ref, c_ref, sel_ref, *rest):
    step = pl.program_id(0)
    blocks = pl.num_programs(0) - LAG
    red_ref = rest[4]
    swap = Exchanger(step, blocks, rest[:4], rest[5:13])
    reducer = Reducer(part_ref, (f0_ref, f1_ref, f2_ref), red_ref, rest[13:])
    swap.before()
    run_stages(reducer, step, None, SECOND_MARKS)

    @pl.when(step < blocks)
    def _():
        select_rows(tab_ref, idsb_ref, sel_ref)
        back = dot_nt(dy_ref[...], sel_ref[...])
        slope = slope_ref[...]
        c = jnp.where(slope != 0.0, slope * back, 0.0)
        c_ref[...] = c
        one, two, three = split3(c)
        tokt = tokt_ref[...]
        grad_t = dot_nn(tokt, one) + dot_nn(tokt, two) + dot_nn(tokt, three)
        place_rows(step, grad_t, ids_ref, step % 2, swap.keep, swap.send)

    swap.after()
    run_stages(reducer, step, pl.num_programs(0) - 1, SECOND_MARKS)


def second_pass(dy, tokt, table, idsb, ids_flip, slope, part, first):
    n_tok, width = dy.shape
    n_list = slope.shape[1]
    cols = OWN_STEP * 128
    steps = n_list // cols
    trows = table.shape[0] // steps
    at = lambda i: jnp.minimum(i, steps - 1)
    row_blk = pl.BlockSpec((cols, width), lambda i: (at(i), 0))
    mat_blk = pl.BlockSpec((n_tok, cols), lambda i: (0, at(i)))
    return pl.pallas_call(
        second_kernel,
        grid=(steps + LAG,),
        in_specs=[
            pl.BlockSpec((n_tok, width), lambda i: (0, 0)),
            pl.BlockSpec((width, n_tok), lambda i: (0, 0)),
            pl.BlockSpec((trows, width), lambda i: (table_block(at(i)), 0)),
            pl.BlockSpec((cols, 128), lambda i: (at(i), 0)),
            pl.BlockSpec(ids_flip.shape, lambda i: (0, 0)),
            mat_blk,
        ] + [pl.BlockSpec(memory_space=pl.ANY)] * 4,
        out_specs=[mat_blk, row_blk] + Exchanger.out_specs(width, steps) + [pl.BlockSpec((128, width), lambda i: (0, 0))],
        out_shape=[
            jax.ShapeDtypeStruct((n_tok, n_list), F32),
            jax.ShapeDtypeStruct((n_list, width), BF16),
        ] + Exchanger.out_shapes(width) + [jax.ShapeDtypeStruct((128, width), BF16)],
        scratch_shapes=Exchanger.scratch(width) + Reducer.scratch(width),
        compiler_params=pltpu.CompilerParams(vmem_limit_bytes=VMEM_LIMIT, has_side_effects=True),
        cost_estimate=pl.CostEstimate(flops=11 * n_tok * n_list * width, bytes_accessed=n_list * (width * 10 + n_tok * 8), transcendentals=0),
        name="second_pass",
    )(dy, tokt, table, idsb, ids_flip, slope, part, *first)


def out_kernel(w_ref, v_ref, c_ref, u_ref, part_ref, f0_ref, f1_ref, f2_ref, y_ref, dx_ref, red_ref, y_acc, dx_acc, *scratch):
    step = pl.program_id(0)
    reducer = Reducer(part_ref, (f0_ref, f1_ref, f2_ref), red_ref, scratch)
    run_stages(reducer, step, None, OUT_MARKS)

    @pl.when(step == 0)
    def _():
        y_acc[...] = jnp.zeros_like(y_acc)
        dx_acc[...] = jnp.zeros_like(dx_acc)

    for mat_ref, row_ref, acc in ((w_ref, v_ref, y_acc), (c_ref, u_ref, dx_acc)):
        one, two, three = split3(mat_ref[...])
        rows = row_ref[...]
        acc[...] += dot_nn(one, rows) + dot_nn(two, rows) + dot_nn(three, rows)

    @pl.when(step == pl.num_programs(0) - 1)
    def _():
        y_ref[...] = y_acc[...].astype(y_ref.dtype)
        dx_ref[...] = dx_acc[...].astype(dx_ref.dtype)

    run_stages(reducer, step, pl.num_programs(0) - 1, OUT_MARKS)


def out_pass(w, v_sel, c, u_sel, part, first):
    n_tok, n_list = w.shape
    width = v_sel.shape[1]
    cols = 512
    mat_blk = pl.BlockSpec((n_tok, cols), lambda i: (0, i))
    row_blk = pl.BlockSpec((cols, width), lambda i: (i, 0))
    whole = pl.BlockSpec((n_tok, width), lambda i: (0, 0))
    return pl.pallas_call(
        out_kernel,
        grid=(n_list // cols,),
        in_specs=[mat_blk, row_blk, mat_blk, row_blk] + [pl.BlockSpec(memory_space=pl.ANY)] * 4,
        out_specs=[whole, whole, pl.BlockSpec((128, width), lambda i: (0, 0))],
        out_shape=[jax.ShapeDtypeStruct((n_tok, width), BF16)] * 2 + [jax.ShapeDtypeStruct((128, width), BF16)],
        scratch_shapes=[pltpu.VMEM((n_tok, width), F32)] * 2 + Reducer.scratch(width),
        compiler_params=pltpu.CompilerParams(vmem_limit_bytes=VMEM_LIMIT, has_side_effects=True),
        cost_estimate=pl.CostEstimate(flops=12 * n_tok * n_list * width, bytes_accessed=n_list * (width * 4 + n_tok * 8), transcendentals=0),
        name="out_pass",
    )(w, v_sel, c, u_sel, part, *first)


def solution(mesh):
    table_n = mesh.shape['table']
    tok_spec = P(('replica', 'data', 'table'))
    row_spec = P(('replica', 'table'))

    def device_step(tok, dy, u_loc, v_loc, wanted, pick, gate):
        n_local, width = u_loc.shape
        half = n_local // 2
        n_tok = tok.shape[0]
        core = lax.axis_index('data')
        me = lax.axis_index('table')
        own_rows = lambda arr: lax.dynamic_slice_in_dim(arr, core * half, half, 0)
        full_u = lax.all_gather(own_rows(u_loc), ('table', 'data'), axis=0, tiled=True)
        full_v = lax.all_gather(own_rows(v_loc), ('table', 'data'), axis=0, tiled=True)

        owners = jnp.arange(table_n, dtype=jnp.int32) ^ me
        ids = jnp.take(wanted.reshape(table_n, -1), owners, axis=0, mode='clip') - owners[:, None] * n_local
        ids_flip = ids ^ (core * half)
        idsb = jnp.broadcast_to(ids.reshape(-1, 1), (ids.size, 128))
        pick_rel = pick.reshape(n_tok, -1) ^ (me << 7)
        gates = gate_matrix(pick_rel, gate.reshape(n_tok, -1), table_n)

        both_cores = lambda rows: lax.all_gather(rows, 'data', axis=0, tiled=True)
        w, slope, u_sel, part_v, *first_v = first_pass(tok, dy.T, full_u, idsb, ids_flip, gates)
        c, v_sel, part_u, *first_u, red_v = second_pass(dy, tok.T, full_v, idsb, ids_flip, slope, part_v, first_v)
        y, dx, red_u = out_pass(w, v_sel, c, u_sel, part_u, first_u)
        grad_v = both_cores(red_v)
        grad_u = both_cores(red_u)
        return y, dx, grad_u, grad_v

    return jax.shard_map(device_step, mesh=mesh, in_specs=(tok_spec, tok_spec, row_spec, row_spec, tok_spec, tok_spec, tok_spec), out_specs=(tok_spec, tok_spec, row_spec, row_spec), check_vma=False)
```

```python
import functools
import jax
import jax.numpy as jnp
from jax import lax
from jax.experimental import pallas as pl
from jax.experimental.pallas import tpu as pltpu
from jax.sharding import PartitionSpec as P

F32 = jnp.float32
BF16 = jnp.bfloat16
SIDE = 4
OWN_STEP = 4
VMEM_LIMIT = 60 * 1024 * 1024
ROW_CUTS = (0, 48, 96, 128)
AXIS_ORDERS = ((2, 1, 0), (1, 0, 2), (0, 2, 1))


def split3(val):
    one = val.astype(BF16)
    rest = val - one.astype(F32)
    two = rest.astype(BF16)
    rest = rest - two.astype(F32)
    return one, two, rest.astype(BF16)


def dot_nn(lhs, rhs):
    return lax.dot_general(lhs, rhs, (((1,), (0,)), ((), ())), preferred_element_type=F32)


def dot_nt(lhs, rhs):
    return lax.dot_general(lhs, rhs, (((1,), (1,)), ((), ())), preferred_element_type=F32)


def select_rows(tab_ref, idsb_ref, sel_ref):
    n_rows = tab_ref.shape[0] // OWN_STEP
    iota = lax.broadcasted_iota(jnp.int32, (128, 128), 1)
    for j in range(OWN_STEP):
        ids = idsb_ref[j * 128:(j + 1) * 128, :]
        hot = jnp.concatenate([jnp.where(ids == iota + 128 * h, 1.0, 0.0).astype(BF16) for h in range(n_rows // 128)], axis=1)
        sel_ref[j * 128:(j + 1) * 128, :] = dot_nn(hot, tab_ref[j * n_rows:(j + 1) * n_rows, :]).astype(BF16)


def place_rows(blk, grad_t, ids_ref, slot, keep_ref, send_ref):
    iota = lax.broadcasted_iota(jnp.int32, (256, 128), 0)
    grad_b = grad_t.astype(BF16)
    for j in range(OWN_STEP):
        hot = jnp.where(iota == ids_ref[pl.ds(blk * OWN_STEP + j, 1), :], 1.0, 0.0).astype(BF16)
        rows = dot_nt(hot, grad_b[:, j * 128:(j + 1) * 128]).astype(BF16)
        keep_ref[slot, j] = rows[:128]
        send_ref[slot, j] = rows[128:]


LAG = 3


class Exchanger:
    @staticmethod
    def scratch(width):
        blk = (2, OWN_STEP, 128, width)
        dma = pltpu.SemaphoreType.DMA
        return [pltpu.VMEM(blk, BF16)] * 4 + [dma((2,)), dma((2,)), dma((2,)), dma((6,)), dma((6,))]

    @staticmethod
    def out_shapes(width):
        rows = [ROW_CUTS[k + 1] - ROW_CUTS[k] for k in range(3)]
        cube = jax.ShapeDtypeStruct((SIDE, SIDE, SIDE, 128, width), BF16)
        return [cube] + [jax.ShapeDtypeStruct((2, SIDE, SIDE, n, width), BF16) for n in rows]

    @staticmethod
    def out_specs():
        return [pl.BlockSpec(memory_space=pl.ANY)] * 4

    def __init__(self, step, blocks, outs, scratch):
        self.step, self.blocks = step, blocks
        self.part_ref, self.first = outs[0], outs[1:]
        self.keep, self.send, self.got, self.sum = scratch[:4]
        self.pair_send, self.pair_recv, self.store_sem, self.out_send, self.out_recv = scratch[4:]
        self.ring = Ring()

    def pair_copy(self, slot):
        other = 1 - lax.axis_index('data')
        return pltpu.make_async_remote_copy(src_ref=self.send.at[slot], dst_ref=self.got.at[slot], send_sem=self.pair_send.at[slot], recv_sem=self.pair_recv.at[slot], device_id={'data': other}, device_id_type=pl.DeviceIdType.MESH)

    def store_copy(self, blk):
        slot = blk % 2
        return pltpu.make_async_copy(self.sum.at[slot], self.part_ref.at[blk // SIDE, blk % SIDE], self.store_sem.at[slot])

    def start_first(self, blk):
        spots = (blk // SIDE, blk % SIDE)
        near = self.ring.near
        for k in range(3):
            axis = AXIS_ORDERS[k][0]
            rows = pl.ds(ROW_CUTS[k], ROW_CUTS[k + 1] - ROW_CUTS[k])
            for way, mark in enumerate((near, 2)):
                def start(k=k, axis=axis, rows=rows, way=way, mark=mark):
                    if axis == 2:
                        src, dst = self.part_ref.at[spots[0], spots[1], mark, rows], self.first[k].at[way, spots[0], spots[1]]
                    else:
                        src, dst = self.part_ref.at[spots[0], spots[1], :, rows], self.first[k].at[way, spots[1 - axis]]
                    pltpu.make_async_remote_copy(src_ref=src, dst_ref=dst, send_sem=self.out_send.at[2 * k + way], recv_sem=self.out_recv.at[2 * k + way], device_id={'table': self.ring.partner(axis, True)}, device_id_type=pl.DeviceIdType.MESH).start()
                if axis == 2:
                    start()
                else:
                    pl.when(spots[axis] == mark)(start)

    def before(self):
        step, blocks = self.step, self.blocks

        @pl.when((step >= 3) & (step - 3 < blocks))
        def _():
            self.store_copy(step - 3).wait()
            self.start_first(step - 3)

        @pl.when((step >= 2) & (step - 2 < blocks))
        def _():
            slot = step % 2
            copy = self.pair_copy(slot)
            copy.wait_recv()
            for j in range(OWN_STEP):
                self.sum[slot, j] = (self.keep[slot, j].astype(F32) + self.got[slot, j].astype(F32)).astype(BF16)
            self.store_copy(step - 2).start()
            copy.wait_send()

        @pl.when((step >= 1) & (step - 1 < blocks))
        def _():
            self.pair_copy((step - 1) % 2).start()

    def after(self):
        @pl.when(self.step == self.blocks + LAG - 1)
        def _():
            for k in range(3):
                for way in range(2):
                    dst = self.first[k].at[way]
                    pltpu.make_async_copy(dst, dst, self.out_send.at[2 * k + way]).wait()
                    pltpu.make_async_copy(dst, dst, self.out_recv.at[2 * k + way]).wait()


class Ring:
    def __init__(self):
        self.core = lax.axis_index('data')
        self.near, self.far = 1 + 2 * self.core, 3 - 2 * self.core

    def partner(self, axis, first):
        me = lax.axis_index('table')
        stride = SIDE ** (2 - axis)
        pos = (me // stride) % SIDE
        even, odd = pos + 1 - 2 * (pos % 2), 3 - pos
        new = even + self.core * (odd - even) if first else odd + self.core * (even - odd)
        return me + (new - pos) * stride


class Gatherer(Ring):
    STEPS = {1: (0,), 2: (1, 2), 3: (3,), 4: (4, 5), 5: (6,), 6: (7, 8)}

    @staticmethod
    def scratch():
        return [pltpu.SemaphoreType.DMA((27,))] * 4 + [pltpu.SemaphoreType.DMA((1,))]

    def __init__(self, own, full, scratch):
        super().__init__()
        self.own, self.full = own, full
        self.send_sem, self.recv_sem, self.pass_send, self.pass_recv, self.own_sem = scratch

    def spot(self, k, ia, ib, ic):
        idx = [None] * 3
        for axis, val in zip(AXIS_ORDERS[k], (ia, ib, ic)):
            idx[axis] = val
        start = pl.multiple_of(self.core * 128 + ROW_CUTS[k], 16)
        return self.full.at[idx[0], idx[1], idx[2], pl.ds(start, ROW_CUTS[k + 1] - ROW_CUTS[k])]

    def ends(self, num):
        near, far, every = self.near, self.far, slice(None)
        return (
            ((0, 0, 0), (near, 0, 0)),
            ((0, 0, 0), (far, 0, 0)),
            ((near, 0, 0), (2, 0, 0)),
            ((every, 0, 0), (every, near, 0)),
            ((every, 0, 0), (every, far, 0)),
            ((every, near, 0), (every, 2, 0)),
            ((every, every, 0), (every, every, near)),
            ((every, every, 0), (every, every, far)),
            ((every, every, near), (every, every, 2)),
        )[num]

    def copy(self, k, num):
        src, dst = self.ends(num)
        step = [key for key, nums in self.STEPS.items() if num in nums][0]
        at = 9 * k + num
        there = self.partner(AXIS_ORDERS[k][(step - 1) // 2], step % 2 == 1)
        return pltpu.make_async_remote_copy(src_ref=self.spot(k, *src), dst_ref=self.spot(k, *dst), send_sem=self.send_sem.at[at], recv_sem=self.recv_sem.at[at], device_id={'table': there}, device_id_type=pl.DeviceIdType.MESH)

    def forward(self, k, num):
        here = self.spot(k, *self.ends(num)[1])
        at = 9 * k + num
        return pltpu.make_async_remote_copy(src_ref=here, dst_ref=here, send_sem=self.pass_send.at[at], recv_sem=self.pass_recv.at[at], device_id={'data': 1 - self.core}, device_id_type=pl.DeviceIdType.MESH)

    def begin(self):
        own = pltpu.make_async_copy(self.own, self.full.at[0, 0, 0], self.own_sem.at[0])
        own.start()
        own.wait()

    def send(self, step):
        for k in range(3):
            for num in self.STEPS[step]:
                self.copy(k, num).start()

    def arrive(self, *nums):
        for k in range(3):
            for num in nums:
                self.copy(k, num).wait_recv()

    def spread(self, *nums):
        for k in range(3):
            for num in nums:
                self.forward(k, num).start()

    def finish(self, *nums):
        for k in range(3):
            for num in nums:
                self.copy(k, num).wait_send()
                self.forward(k, num).wait_send()
                self.forward(k, num).wait_recv()


GATE_STEPS = 16


def gate_kernel(n_own, pick_ref, gate_ref, u_ref, v_ref, out_ref, full_u_ref, full_v_ref, tile_ref, *scratch):
    step = pl.program_id(0)
    get_u = Gatherer(u_ref, full_u_ref, scratch[:5])
    get_v = Gatherer(v_ref, full_v_ref, scratch[5:])

    @pl.when(step == 0)
    def _():
        for get in (get_u, get_v):
            get.begin()
            get.send(1)

    for mark, got, then in ((3, (0,), 2), (6, (1, 2), 3), (10, (3,), 4)):
        @pl.when(step == mark)
        def _(got=got, then=then):
            for get in (get_u, get_v):
                get.arrive(*got)
                get.send(then)
                get.spread(*got)

    @pl.when(step == GATE_STEPS - 1)
    def _():
        get_u.arrive(4, 5)
        get_u.send(5)
        get_u.spread(4, 5)

    sel = pick_ref.shape[1]
    iota_own = lax.broadcasted_iota(jnp.int32, (n_own, sel), 0)
    iota_lo = lax.broadcasted_iota(jnp.int32, (128, sel), 0)

    def body(grp, carry):
        base = pl.multiple_of(grp * 8, 8)
        pick = pick_ref[pl.ds(base, 8), :]
        hi = pick >> 7
        lo = pick & 127
        parts = [piece.astype(F32) for piece in split3(gate_ref[pl.ds(base, 8), :])]
        for j in range(8):
            mask = iota_own == hi[j:j + 1, :]
            left = jnp.concatenate([jnp.where(mask, piece[j:j + 1, :], 0.0).astype(BF16) for piece in parts], axis=0)
            right = jnp.where(iota_lo == lo[j:j + 1, :], 1.0, 0.0).astype(BF16)
            res = dot_nt(left, right)
            tile_ref[j * n_own:(j + 1) * n_own, :] = res[:n_own] + res[n_own:2 * n_own] + res[2 * n_own:]
        for o in range(n_own):
            out_ref[pl.ds(base, 8), o * 128:(o + 1) * 128] = tile_ref[pl.ds(o, 8, stride=n_own), :]
        return carry

    lax.fori_loop(0, pick_ref.shape[0] // 8, body, 0)

    @pl.when(step == GATE_STEPS - 1)
    def _():
        get_v.arrive(4, 5)
        get_v.spread(4, 5)
        get_u.arrive(6)
        get_u.send(6)
        get_u.spread(6)
        get_v.finish(0, 1, 2, 3, 4, 5)
        get_u.arrive(7)
        get_u.spread(7)
        get_u.arrive(8)
        get_u.spread(8)
        get_u.finish(0, 1, 2, 3, 4, 5, 6, 7, 8)


def gate_matrix(pick_rel, gate, u_loc, v_loc, n_own):
    tok, sel = pick_rel.shape
    blk = tok // GATE_STEPS
    own = pl.BlockSpec(u_loc.shape, lambda i: (0, 0))
    full = jax.ShapeDtypeStruct((SIDE, SIDE, SIDE) + u_loc.shape, BF16)
    return pl.pallas_call(
        functools.partial(gate_kernel, n_own),
        grid=(GATE_STEPS,),
        in_specs=[pl.BlockSpec((blk, sel), lambda i: (i, 0)), pl.BlockSpec((blk, sel), lambda i: (i, 0)), own, own],
        out_specs=[pl.BlockSpec((blk, n_own * 128), lambda i: (i, 0))] + [pl.BlockSpec(memory_space=pl.ANY)] * 2,
        out_shape=[jax.ShapeDtypeStruct((tok, n_own * 128), F32), full, full],
        scratch_shapes=[pltpu.VMEM((8 * n_own, 128), F32)] + Gatherer.scratch() + Gatherer.scratch(),
        compiler_params=pltpu.CompilerParams(vmem_limit_bytes=VMEM_LIMIT, has_side_effects=True),
        cost_estimate=pl.CostEstimate(flops=2 * tok * 256 * 256 * 192, bytes_accessed=tok * n_own * 512, transcendentals=0),
        name="gate_matrix",
    )(pick_rel, gate, u_loc, v_loc)


def first_kernel(tok_ref, dyt_ref, tab_ref, idsb_ref, ids_ref, gate_ref, held_ref, w_ref, slope_ref, sel_ref, full_ref, *rest):
    step = pl.program_id(0)
    blocks = pl.num_programs(0) - LAG
    swap = Exchanger(step, blocks, rest[:4], rest[4:13])
    get_v = Gatherer(None, full_ref, rest[13:])

    @pl.when(step == 0)
    def _():
        get_v.send(5)

    @pl.when(step == 5)
    def _():
        get_v.arrive(6)
        get_v.send(6)
        get_v.spread(6)

    @pl.when(step == 12)
    def _():
        get_v.arrive(7)
        get_v.spread(7)

    swap.before()

    @pl.when(step < blocks)
    def _():
        select_rows(tab_ref, idsb_ref, sel_ref)
        pre = dot_nt(tok_ref[...], sel_ref[...])
        gate = gate_ref[...]
        cdf = 0.5 * (1.0 + lax.erf(pre * 0.7071067811865476))
        pdf = jnp.exp(-0.5 * pre * pre) * 0.3989422804014327
        live = gate != 0.0
        w = jnp.where(live, gate * (pre * cdf), 0.0)
        w_ref[...] = w
        slope_ref[...] = jnp.where(live, gate * (cdf + pre * pdf), 0.0)
        one, two, three = split3(w)
        dyt = dyt_ref[...]
        grad_t = dot_nn(dyt, one) + dot_nn(dyt, two) + dot_nn(dyt, three)
        place_rows(step, grad_t, ids_ref, step % 2, swap.keep, swap.send)

    @pl.when(step == blocks + LAG - 1)
    def _():
        get_v.arrive(8)
        get_v.spread(8)

    swap.after()

    @pl.when(step == blocks + LAG - 1)
    def _():
        get_v.finish(6, 7, 8)


def first_pass(tok, dyt, table, idsb, ids_flip, gate, held):
    n_tok, width = tok.shape
    n_list = gate.shape[1]
    cols = OWN_STEP * 128
    steps = n_list // cols
    trows = table.shape[0] // steps
    at = lambda i: jnp.minimum(i, steps - 1)
    row_blk = pl.BlockSpec((cols, width), lambda i: (at(i), 0))
    mat_blk = pl.BlockSpec((n_tok, cols), lambda i: (0, at(i)))
    return pl.pallas_call(
        first_kernel,
        grid=(steps + LAG,),
        in_specs=[
            pl.BlockSpec((n_tok, width), lambda i: (0, 0)),
            pl.BlockSpec((width, n_tok), lambda i: (0, 0)),
            pl.BlockSpec((trows, width), lambda i: (at(i), 0)),
            pl.BlockSpec((cols, 128), lambda i: (at(i), 0)),
            pl.BlockSpec(ids_flip.shape, lambda i: (0, 0)),
            mat_blk,
            pl.BlockSpec(memory_space=pl.ANY),
        ],
        out_specs=[mat_blk, mat_blk, row_blk, pl.BlockSpec(memory_space=pl.ANY)] + Exchanger.out_specs(),
        out_shape=[
            jax.ShapeDtypeStruct((n_tok, n_list), F32),
            jax.ShapeDtypeStruct((n_tok, n_list), F32),
            jax.ShapeDtypeStruct((n_list, width), BF16),
            jax.ShapeDtypeStruct(held.shape, BF16),
        ] + Exchanger.out_shapes(width),
        scratch_shapes=Exchanger.scratch(width) + Gatherer.scratch(),
        input_output_aliases={6: 3},
        compiler_params=pltpu.CompilerParams(vmem_limit_bytes=VMEM_LIMIT, has_side_effects=True),
        cost_estimate=pl.CostEstimate(flops=11 * n_tok * n_list * width, bytes_accessed=n_list * (width * 10 + n_tok * 12), transcendentals=0),
        name="first_pass",
    )(tok, dyt, table, idsb, ids_flip, gate, held)


class Reducer(Ring):
    N_COPIES = 9

    @staticmethod
    def scratch(width):
        shapes = []
        for k in range(3):
            rows = ROW_CUTS[k + 1] - ROW_CUTS[k]
            lead = [(2, SIDE, SIDE), (2, SIDE, SIDE), (SIDE, SIDE), (2, SIDE), (SIDE,), (2,), (1,)]
            shapes += [pltpu.VMEM(dims + (rows, width), BF16) for dims in lead]
        return shapes + [pltpu.SemaphoreType.DMA((27,)), pltpu.SemaphoreType.DMA((27,)), pltpu.SemaphoreType.DMA((12,))]

    def __init__(self, src, first, out, scratch):
        super().__init__()
        self.src, self.first, self.out = src, first, out
        self.bufs = [scratch[7 * k:7 * k + 7] for k in range(3)]
        self.send_sem, self.recv_sem, self.load_sem = scratch[21:]

    def remote(self, k, num, src, dst, axis, first):
        at = k * self.N_COPIES + num
        return pltpu.make_async_remote_copy(src_ref=src, dst_ref=dst, send_sem=self.send_sem.at[at], recv_sem=self.recv_sem.at[at], device_id={'table': self.partner(axis, first)}, device_id_type=pl.DeviceIdType.MESH)

    def slab(self, k, slot):
        idx = [slice(None)] * 3
        idx[AXIS_ORDERS[k][0]] = slot
        return self.src.at[idx[0], idx[1], idx[2], pl.ds(ROW_CUTS[k], ROW_CUTS[k + 1] - ROW_CUTS[k])]

    def order(self, k, b, c):
        return (b, c) if AXIS_ORDERS[k][1] < AXIS_ORDERS[k][2] else (c, b)

    def loads(self):
        own = [pltpu.make_async_copy(self.slab(k, slot), self.bufs[k][0].at[j], self.load_sem.at[2 * k + j]) for j, slot in ((1, self.far), (0, 0)) for k in range(3)]
        come = [pltpu.make_async_copy(self.first[k].at[j], self.bufs[k][1].at[j], self.load_sem.at[6 + 2 * k + j]) for j in (1, 0) for k in range(3)]
        return [copy for j in range(2) for copy in own[3 * j:3 * j + 3] + come[3 * j:3 * j + 3]]

    def copies(self, stage):
        out = []
        for k in range(3):
            a, b, c = AXIS_ORDERS[k]
            held, got1, got2, got3, got4, got5, got6 = self.bufs[k]
            if stage == 2:
                out.append(self.remote(k, 2, held.at[1], got2, a, False))
            elif stage == 3:
                out += [self.remote(k, 3 + j, self.row_of(k, held, slot), got3.at[j], b, True) for j, slot in enumerate((self.near, 2))]
            elif stage == 4:
                out.append(self.remote(k, 5, self.row_of(k, held, self.far), got4, b, False))
            elif stage == 5:
                out += [self.remote(k, 6 + j, held.at[(0,) + self.order(k, 0, slot)], got5.at[j], c, True) for j, slot in enumerate((self.near, 2))]
            else:
                out.append(self.remote(k, 8, held.at[(0,) + self.order(k, 0, self.far)], got6.at[0], c, False))
        return out

    def row_of(self, k, held, slot):
        p, q = self.order(k, slot, slice(None))
        return held.at[0, p, q]

    def terms(self, k, b, c, depth):
        held, got1, got2, got3, got4, got5, got6 = self.bufs[k]
        p, q = self.order(k, b, c)
        arrs = [held[0, p, q], got1[0, p, q], got2[p, q]]
        return p, q, arrs

    def total(self, arrs):
        return functools.reduce(jnp.add, [arr.astype(F32) for arr in arrs])

    def add(self, stage):
        for k in range(3):
            held, got1, got2, got3, got4, got5, got6 = self.bufs[k]
            if stage == 2:
                def body(i, carry):
                    p, q = i // SIDE, i % SIDE
                    held[1, p, q] = self.total([held[1, p, q], got1[1, p, q]]).astype(BF16)
                    return carry
                lax.fori_loop(0, SIDE * SIDE, body, 0)
            elif stage == 3:
                def body(i, carry):
                    j = i // SIDE
                    p, q, arrs = self.terms(k, self.near + j * (2 - self.near), i % SIDE, 3)
                    held[0, p, q] = self.total(arrs).astype(BF16)
                    return carry
                lax.fori_loop(0, 2 * SIDE, body, 0)
            elif stage == 4:
                def body(c, carry):
                    p, q, arrs = self.terms(k, self.far, c, 4)
                    held[0, p, q] = self.total(arrs + [got3[1, c]]).astype(BF16)
                    return carry
                lax.fori_loop(0, SIDE, body, 0)
            elif stage == 5:
                for slot in (self.near, 2):
                    p, q, arrs = self.terms(k, 0, slot, 5)
                    held[0, p, q] = self.total(arrs + [got3[0, slot], got4[slot]]).astype(BF16)
            elif stage == 6:
                p, q, arrs = self.terms(k, 0, self.far, 6)
                held[0, p, q] = self.total(arrs + [got3[0, self.far], got4[self.far], got5[1]]).astype(BF16)
            else:
                p, q, arrs = self.terms(k, 0, 0, 7)
                self.out[ROW_CUTS[k]:ROW_CUTS[k + 1], :] = self.total(arrs + [got3[0, 0], got4[0], got5[0], got6[0]]).astype(self.out.dtype)

    def run(self, stage):
        if stage == 1:
            for copy in self.loads():
                copy.start()
            return
        if stage == 2:
            for copy in self.loads():
                copy.wait()
        else:
            for copy in self.copies(stage - 1):
                copy.wait_recv()
        self.add(stage)
        if stage < 7:
            for copy in self.copies(stage):
                copy.start()
        else:
            for done in range(2, 7):
                for copy in self.copies(done):
                    copy.wait_send()


def run_stages(reducer, step, last, marks):
    for stage, mark in marks:
        if last is None and mark is not None:
            pl.when(step == mark)(functools.partial(reducer.run, stage))
    if last is not None:
        @pl.when(step == last)
        def _():
            for stage, mark in marks:
                if mark is None:
                    reducer.run(stage)


SECOND_MARKS = ((1, 0), (2, 2), (3, 8), (4, 12), (5, 14), (6, 16), (7, None))
OUT_MARKS = ((1, 0), (2, 2), (3, 8), (4, 11), (5, 13), (6, 15), (7, None))


def second_kernel(dy_ref, tokt_ref, tab_ref, idsb_ref, ids_ref, slope_ref, part_ref, f0_ref, f1_ref, f2_ref, c_ref, sel_ref, *rest):
    step = pl.program_id(0)
    blocks = pl.num_programs(0) - LAG
    red_ref = rest[4]
    swap = Exchanger(step, blocks, rest[:4], rest[5:14])
    reducer = Reducer(part_ref, (f0_ref, f1_ref, f2_ref), red_ref, rest[14:])
    swap.before()
    run_stages(reducer, step, None, SECOND_MARKS)

    @pl.when(step < blocks)
    def _():
        select_rows(tab_ref, idsb_ref, sel_ref)
        back = dot_nt(dy_ref[...], sel_ref[...])
        slope = slope_ref[...]
        c = jnp.where(slope != 0.0, slope * back, 0.0)
        c_ref[...] = c
        one, two, three = split3(c)
        tokt = tokt_ref[...]
        grad_t = dot_nn(tokt, one) + dot_nn(tokt, two) + dot_nn(tokt, three)
        place_rows(step, grad_t, ids_ref, step % 2, swap.keep, swap.send)

    swap.after()
    run_stages(reducer, step, pl.num_programs(0) - 1, SECOND_MARKS)


def second_pass(dy, tokt, table, idsb, ids_flip, slope, part, first):
    n_tok, width = dy.shape
    n_list = slope.shape[1]
    cols = OWN_STEP * 128
    steps = n_list // cols
    trows = table.shape[0] // steps
    at = lambda i: jnp.minimum(i, steps - 1)
    row_blk = pl.BlockSpec((cols, width), lambda i: (at(i), 0))
    mat_blk = pl.BlockSpec((n_tok, cols), lambda i: (0, at(i)))
    return pl.pallas_call(
        second_kernel,
        grid=(steps + LAG,),
        in_specs=[
            pl.BlockSpec((n_tok, width), lambda i: (0, 0)),
            pl.BlockSpec((width, n_tok), lambda i: (0, 0)),
            pl.BlockSpec((trows, width), lambda i: (at(i), 0)),
            pl.BlockSpec((cols, 128), lambda i: (at(i), 0)),
            pl.BlockSpec(ids_flip.shape, lambda i: (0, 0)),
            mat_blk,
        ] + [pl.BlockSpec(memory_space=pl.ANY)] * 4,
        out_specs=[mat_blk, row_blk] + Exchanger.out_specs() + [pl.BlockSpec((128, width), lambda i: (0, 0))],
        out_shape=[
            jax.ShapeDtypeStruct((n_tok, n_list), F32),
            jax.ShapeDtypeStruct((n_list, width), BF16),
        ] + Exchanger.out_shapes(width) + [jax.ShapeDtypeStruct((128, width), BF16)],
        scratch_shapes=Exchanger.scratch(width) + Reducer.scratch(width),
        compiler_params=pltpu.CompilerParams(vmem_limit_bytes=VMEM_LIMIT, has_side_effects=True),
        cost_estimate=pl.CostEstimate(flops=11 * n_tok * n_list * width, bytes_accessed=n_list * (width * 10 + n_tok * 8), transcendentals=0),
        name="second_pass",
    )(dy, tokt, table, idsb, ids_flip, slope, part, *first)


def out_kernel(w_ref, v_ref, c_ref, u_ref, part_ref, f0_ref, f1_ref, f2_ref, y_ref, dx_ref, red_ref, y_acc, dx_acc, *scratch):
    step = pl.program_id(0)
    reducer = Reducer(part_ref, (f0_ref, f1_ref, f2_ref), red_ref, scratch)
    run_stages(reducer, step, None, OUT_MARKS)

    @pl.when(step == 0)
    def _():
        y_acc[...] = jnp.zeros_like(y_acc)
        dx_acc[...] = jnp.zeros_like(dx_acc)

    for mat_ref, row_ref, acc in ((w_ref, v_ref, y_acc), (c_ref, u_ref, dx_acc)):
        one, two, three = split3(mat_ref[...])
        rows = row_ref[...]
        acc[...] += dot_nn(one, rows) + dot_nn(two, rows) + dot_nn(three, rows)

    @pl.when(step == pl.num_programs(0) - 1)
    def _():
        y_ref[...] = y_acc[...].astype(y_ref.dtype)
        dx_ref[...] = dx_acc[...].astype(dx_ref.dtype)

    run_stages(reducer, step, pl.num_programs(0) - 1, OUT_MARKS)


def out_pass(w, v_sel, c, u_sel, part, first):
    n_tok, n_list = w.shape
    width = v_sel.shape[1]
    cols = 512
    mat_blk = pl.BlockSpec((n_tok, cols), lambda i: (0, i))
    row_blk = pl.BlockSpec((cols, width), lambda i: (i, 0))
    whole = pl.BlockSpec((n_tok, width), lambda i: (0, 0))
    return pl.pallas_call(
        out_kernel,
        grid=(n_list // cols,),
        in_specs=[mat_blk, row_blk, mat_blk, row_blk] + [pl.BlockSpec(memory_space=pl.ANY)] * 4,
        out_specs=[whole, whole, pl.BlockSpec((128, width), lambda i: (0, 0))],
        out_shape=[jax.ShapeDtypeStruct((n_tok, width), BF16)] * 2 + [jax.ShapeDtypeStruct((128, width), BF16)],
        scratch_shapes=[pltpu.VMEM((n_tok, width), F32)] * 2 + Reducer.scratch(width),
        compiler_params=pltpu.CompilerParams(vmem_limit_bytes=VMEM_LIMIT, has_side_effects=True),
        cost_estimate=pl.CostEstimate(flops=12 * n_tok * n_list * width, bytes_accessed=n_list * (width * 4 + n_tok * 8), transcendentals=0),
        name="out_pass",
    )(w, v_sel, c, u_sel, part, *first)


def solution(mesh):
    table_n = mesh.shape['table']
    tok_spec = P(('replica', 'data', 'table'))
    row_spec = P(('replica', 'table'))

    def device_step(tok, dy, u_loc, v_loc, wanted, pick, gate):
        n_local, width = u_loc.shape
        half = n_local // 2
        n_tok = tok.shape[0]
        core = lax.axis_index('data')
        me = lax.axis_index('table')
        owners = jnp.arange(table_n, dtype=jnp.int32) ^ me
        ids = jnp.take(wanted.reshape(table_n, -1), owners, axis=0, mode='clip') - owners[:, None] * n_local
        ids_flip = ids ^ (core * half)
        idsb = jnp.broadcast_to(ids.reshape(-1, 1), (ids.size, 128))
        pick_rel = pick.reshape(n_tok, -1) ^ (me << 7)
        gates, full_u, full_v = gate_matrix(pick_rel, gate.reshape(n_tok, -1), u_loc, v_loc, table_n)
        flat = lambda full: full.reshape(table_n * n_local, width)

        both_cores = lambda rows: lax.all_gather(rows, 'data', axis=0, tiled=True)
        w, slope, u_sel, full_v, part_v, *first_v = first_pass(tok, dy.T, flat(full_u), idsb, ids_flip, gates, full_v)
        c, v_sel, part_u, *first_u, red_v = second_pass(dy, tok.T, flat(full_v), idsb, ids_flip, slope, part_v, first_v)
        y, dx, red_u = out_pass(w, v_sel, c, u_sel, part_u, first_u)
        grad_v = both_cores(red_v)
        grad_u = both_cores(red_u)
        return y, dx, grad_u, grad_v

    return jax.shard_map(device_step, mesh=mesh, in_specs=(tok_spec, tok_spec, row_spec, row_spec, tok_spec, tok_spec, tok_spec), out_specs=(tok_spec, tok_spec, row_spec, row_spec), check_vma=False)
```

```python
import functools
import jax
import jax.numpy as jnp
from jax import lax
from jax.experimental import pallas as pl
from jax.experimental.pallas import tpu as pltpu
from jax.sharding import PartitionSpec as P

F32 = jnp.float32
BF16 = jnp.bfloat16
SIDE = 4
OWN_STEP = 4
VMEM_LIMIT = 60 * 1024 * 1024
ROW_CUTS = (0, 48, 88, 128)
AXIS_ORDERS = ((2, 1, 0), (1, 0, 2), (0, 2, 1))


def split3(val):
    one = val.astype(BF16)
    rest = val - one.astype(F32)
    two = rest.astype(BF16)
    rest = rest - two.astype(F32)
    return one, two, rest.astype(BF16)


def dot_nn(lhs, rhs):
    return lax.dot_general(lhs, rhs, (((1,), (0,)), ((), ())), preferred_element_type=F32)


def dot_nt(lhs, rhs):
    return lax.dot_general(lhs, rhs, (((1,), (1,)), ((), ())), preferred_element_type=F32)


def select_rows(tab_ref, idsb_ref, sel_ref):
    n_rows = tab_ref.shape[0] // OWN_STEP
    iota = lax.broadcasted_iota(jnp.int32, (128, 128), 1)
    for j in range(OWN_STEP):
        ids = idsb_ref[j * 128:(j + 1) * 128, :]
        hot = jnp.concatenate([jnp.where(ids == iota + 128 * h, 1.0, 0.0).astype(BF16) for h in range(n_rows // 128)], axis=1)
        sel_ref[j * 128:(j + 1) * 128, :] = dot_nn(hot, tab_ref[j * n_rows:(j + 1) * n_rows, :]).astype(BF16)


def place_rows(blk, grad_t, ids_ref, slot, keep_ref, send_ref):
    iota = lax.broadcasted_iota(jnp.int32, (256, 128), 0)
    grad_b = grad_t.astype(BF16)
    for j in range(OWN_STEP):
        hot = jnp.where(iota == ids_ref[pl.ds(blk * OWN_STEP + j, 1), :], 1.0, 0.0).astype(BF16)
        rows = dot_nt(hot, grad_b[:, j * 128:(j + 1) * 128]).astype(BF16)
        keep_ref[slot, j] = rows[:128]
        send_ref[slot, j] = rows[128:]


LAG = 3


class Exchanger:
    @staticmethod
    def scratch(width):
        blk = (2, OWN_STEP, 128, width)
        dma = pltpu.SemaphoreType.DMA
        return [pltpu.VMEM(blk, BF16)] * 4 + [dma((2,)), dma((2,)), dma((2,)), dma((6,)), dma((6,))]

    @staticmethod
    def out_shapes(width):
        rows = [ROW_CUTS[k + 1] - ROW_CUTS[k] for k in range(3)]
        cube = jax.ShapeDtypeStruct((SIDE, SIDE, SIDE, 128, width), BF16)
        return [cube] + [jax.ShapeDtypeStruct((2, SIDE, SIDE, n, width), BF16) for n in rows]

    @staticmethod
    def out_specs():
        return [pl.BlockSpec(memory_space=pl.ANY)] * 4

    def __init__(self, step, blocks, outs, scratch):
        self.step, self.blocks = step, blocks
        self.part_ref, self.first = outs[0], outs[1:]
        self.keep, self.send, self.got, self.sum = scratch[:4]
        self.pair_send, self.pair_recv, self.store_sem, self.out_send, self.out_recv = scratch[4:]
        self.ring = Ring()

    def pair_copy(self, slot):
        other = 1 - lax.axis_index('data')
        return pltpu.make_async_remote_copy(src_ref=self.send.at[slot], dst_ref=self.got.at[slot], send_sem=self.pair_send.at[slot], recv_sem=self.pair_recv.at[slot], device_id={'data': other}, device_id_type=pl.DeviceIdType.MESH)

    def store_copy(self, blk):
        slot = blk % 2
        return pltpu.make_async_copy(self.sum.at[slot], self.part_ref.at[blk // SIDE, blk % SIDE], self.store_sem.at[slot])

    def start_first(self, blk):
        spots = (blk // SIDE, blk % SIDE)
        near = self.ring.near
        for k in range(3):
            axis = AXIS_ORDERS[k][0]
            rows = pl.ds(ROW_CUTS[k], ROW_CUTS[k + 1] - ROW_CUTS[k])
            for way, mark in enumerate((near, 2)):
                def start(k=k, axis=axis, rows=rows, way=way, mark=mark):
                    if axis == 2:
                        src, dst = self.part_ref.at[spots[0], spots[1], mark, rows], self.first[k].at[way, spots[0], spots[1]]
                    else:
                        src, dst = self.part_ref.at[spots[0], spots[1], :, rows], self.first[k].at[way, spots[1 - axis]]
                    pltpu.make_async_remote_copy(src_ref=src, dst_ref=dst, send_sem=self.out_send.at[2 * k + way], recv_sem=self.out_recv.at[2 * k + way], device_id={'table': self.ring.partner(axis, True)}, device_id_type=pl.DeviceIdType.MESH).start()
                if axis == 2:
                    start()
                else:
                    pl.when(spots[axis] == mark)(start)

    def before(self):
        step, blocks = self.step, self.blocks

        @pl.when((step >= 3) & (step - 3 < blocks))
        def _():
            self.store_copy(step - 3).wait()
            self.start_first(step - 3)

        @pl.when((step >= 2) & (step - 2 < blocks))
        def _():
            slot = step % 2
            copy = self.pair_copy(slot)
            copy.wait_recv()
            for j in range(OWN_STEP):
                self.sum[slot, j] = self.keep[slot, j] + self.got[slot, j]
            self.store_copy(step - 2).start()
            copy.wait_send()

        @pl.when((step >= 1) & (step - 1 < blocks))
        def _():
            self.pair_copy((step - 1) % 2).start()

    def after(self):
        @pl.when(self.step == self.blocks + LAG - 1)
        def _():
            for k in range(3):
                for way in range(2):
                    dst = self.first[k].at[way]
                    pltpu.make_async_copy(dst, dst, self.out_send.at[2 * k + way]).wait()
                    pltpu.make_async_copy(dst, dst, self.out_recv.at[2 * k + way]).wait()


class Ring:
    def __init__(self):
        self.core = lax.axis_index('data')
        self.near, self.far = 1 + 2 * self.core, 3 - 2 * self.core

    def partner(self, axis, first):
        me = lax.axis_index('table')
        stride = SIDE ** (2 - axis)
        pos = (me // stride) % SIDE
        even, odd = pos + 1 - 2 * (pos % 2), 3 - pos
        new = even + self.core * (odd - even) if first else odd + self.core * (even - odd)
        return me + (new - pos) * stride


class Gatherer(Ring):
    STEPS = {1: (0,), 2: (1, 2), 3: (3,), 4: (4, 5), 5: (6,), 6: (7, 8)}

    @staticmethod
    def scratch():
        return [pltpu.SemaphoreType.DMA((27,))] * 4 + [pltpu.SemaphoreType.DMA((1,))]

    def __init__(self, own, full, scratch):
        super().__init__()
        self.own, self.full = own, full
        self.send_sem, self.recv_sem, self.pass_send, self.pass_recv, self.own_sem = scratch

    def spot(self, k, ia, ib, ic):
        idx = [None] * 3
        for axis, val in zip(AXIS_ORDERS[k], (ia, ib, ic)):
            idx[axis] = val
        start = pl.multiple_of(self.core * 128 + ROW_CUTS[k], 8)
        return self.full.at[idx[0], idx[1], idx[2], pl.ds(start, ROW_CUTS[k + 1] - ROW_CUTS[k])]

    def ends(self, num):
        near, far, every = self.near, self.far, slice(None)
        return (
            ((0, 0, 0), (near, 0, 0)),
            ((0, 0, 0), (far, 0, 0)),
            ((near, 0, 0), (2, 0, 0)),
            ((every, 0, 0), (every, near, 0)),
            ((every, 0, 0), (every, far, 0)),
            ((every, near, 0), (every, 2, 0)),
            ((every, every, 0), (every, every, near)),
            ((every, every, 0), (every, every, far)),
            ((every, every, near), (every, every, 2)),
        )[num]

    def copy(self, k, num):
        src, dst = self.ends(num)
        step = [key for key, nums in self.STEPS.items() if num in nums][0]
        at = 9 * k + num
        there = self.partner(AXIS_ORDERS[k][(step - 1) // 2], step % 2 == 1)
        return pltpu.make_async_remote_copy(src_ref=self.spot(k, *src), dst_ref=self.spot(k, *dst), send_sem=self.send_sem.at[at], recv_sem=self.recv_sem.at[at], device_id={'table': there}, device_id_type=pl.DeviceIdType.MESH)

    def forward(self, k, num):
        here = self.spot(k, *self.ends(num)[1])
        at = 9 * k + num
        return pltpu.make_async_remote_copy(src_ref=here, dst_ref=here, send_sem=self.pass_send.at[at], recv_sem=self.pass_recv.at[at], device_id={'data': 1 - self.core}, device_id_type=pl.DeviceIdType.MESH)

    def begin(self):
        own = pltpu.make_async_copy(self.own, self.full.at[0, 0, 0], self.own_sem.at[0])
        own.start()
        own.wait()

    def send(self, step):
        for k in range(3):
            for num in self.STEPS[step]:
                self.copy(k, num).start()

    def arrive(self, *nums):
        for k in range(3):
            for num in nums:
                self.copy(k, num).wait_recv()

    def spread(self, *nums):
        for k in range(3):
            for num in nums:
                self.forward(k, num).start()

    def finish(self, *nums):
        for k in range(3):
            for num in nums:
                self.copy(k, num).wait_send()
                self.forward(k, num).wait_send()
                self.forward(k, num).wait_recv()


GATE_STEPS = 16


def gate_kernel(n_own, pick_ref, gate_ref, ids_ref, u_ref, v_ref, out_ref, idsb_ref, full_u_ref, full_v_ref, tile_ref, *scratch):
    step = pl.program_id(0)
    get_u = Gatherer(u_ref, full_u_ref, scratch[:5])
    get_v = Gatherer(v_ref, full_v_ref, scratch[5:])

    @pl.when(step == 0)
    def _():
        for get in (get_u, get_v):
            get.begin()
            get.send(1)
        for got, then in (((0,), 2), ((1, 2), 3), ((3,), 4)):
            for get in (get_u, get_v):
                get.arrive(*got)
                get.send(then)
                get.spread(*got)
        get_u.arrive(4, 5)
        get_u.send(5)
        get_u.spread(4, 5)

    @pl.when(step == 2)
    def _():
        get_v.arrive(4, 5)
        get_v.spread(4, 5)

    @pl.when(step == 9)
    def _():
        get_u.arrive(6)
        get_u.send(6)
        get_u.spread(6)

    for j in range(OWN_STEP):
        row = ids_ref[pl.ds(step * OWN_STEP + j, 1), :].astype(F32)
        idsb_ref[j * 128:(j + 1) * 128, :] = jnp.transpose(jnp.broadcast_to(row, (128, 128))).astype(jnp.int32)

    sel = pick_ref.shape[1]
    iota_own = lax.broadcasted_iota(jnp.int32, (n_own, sel), 0)
    iota_lo = lax.broadcasted_iota(jnp.int32, (128, sel), 0)

    def body(grp, carry):
        base = pl.multiple_of(grp * 8, 8)
        pick = pick_ref[pl.ds(base, 8), :]
        hi = pick >> 7
        lo = pick & 127
        parts = [piece.astype(F32) for piece in split3(gate_ref[pl.ds(base, 8), :])]
        for j in range(8):
            mask = iota_own == hi[j:j + 1, :]
            left = jnp.concatenate([jnp.where(mask, piece[j:j + 1, :], 0.0).astype(BF16) for piece in parts], axis=0)
            right = jnp.where(iota_lo == lo[j:j + 1, :], 1.0, 0.0).astype(BF16)
            res = dot_nt(left, right)
            tile_ref[j * n_own:(j + 1) * n_own, :] = res[:n_own] + res[n_own:2 * n_own] + res[2 * n_own:]
        for o in range(n_own):
            out_ref[pl.ds(base, 8), o * 128:(o + 1) * 128] = tile_ref[pl.ds(o, 8, stride=n_own), :]
        return carry

    lax.fori_loop(0, pick_ref.shape[0] // 8, body, 0)

    @pl.when(step == GATE_STEPS - 1)
    def _():
        get_v.finish(0, 1, 2, 3, 4, 5)
        get_u.arrive(7)
        get_u.spread(7)
        get_u.arrive(8)
        get_u.spread(8)
        get_u.finish(0, 1, 2, 3, 4, 5, 6, 7, 8)


def gate_matrix(pick_rel, gate, ids, u_loc, v_loc, n_own):
    tok, sel = pick_rel.shape
    blk = tok // GATE_STEPS
    own = pl.BlockSpec(u_loc.shape, lambda i: (0, 0))
    full = jax.ShapeDtypeStruct((SIDE, SIDE, SIDE) + u_loc.shape, BF16)
    return pl.pallas_call(
        functools.partial(gate_kernel, n_own),
        grid=(GATE_STEPS,),
        in_specs=[pl.BlockSpec((blk, sel), lambda i: (i, 0)), pl.BlockSpec((blk, sel), lambda i: (i, 0)), pl.BlockSpec(ids.shape, lambda i: (0, 0)), own, own],
        out_specs=[pl.BlockSpec((blk, n_own * 128), lambda i: (i, 0)), pl.BlockSpec((OWN_STEP * 128, 128), lambda i: (i, 0))] + [pl.BlockSpec(memory_space=pl.ANY)] * 2,
        out_shape=[jax.ShapeDtypeStruct((tok, n_own * 128), F32), jax.ShapeDtypeStruct((n_own * 128, 128), jnp.int32), full, full],
        scratch_shapes=[pltpu.VMEM((8 * n_own, 128), F32)] + Gatherer.scratch() + Gatherer.scratch(),
        compiler_params=pltpu.CompilerParams(vmem_limit_bytes=VMEM_LIMIT, has_side_effects=True),
        cost_estimate=pl.CostEstimate(flops=2 * tok * 256 * 256 * 192, bytes_accessed=tok * n_own * 512, transcendentals=0),
        name="gate_matrix",
    )(pick_rel, gate, ids, u_loc, v_loc)


def first_kernel(tok_ref, dyt_ref, tab_ref, idsb_ref, ids_ref, gate_ref, held_ref, w_ref, slope_ref, sel_ref, full_ref, *rest):
    step = pl.program_id(0)
    blocks = pl.num_programs(0) - LAG
    swap = Exchanger(step, blocks, rest[:4], rest[4:13])
    get_v = Gatherer(None, full_ref, rest[13:])

    @pl.when(step == 0)
    def _():
        get_v.send(5)

    @pl.when(step == 6)
    def _():
        get_v.arrive(6)
        get_v.send(6)
        get_v.spread(6)

    @pl.when(step == 13)
    def _():
        get_v.arrive(7)
        get_v.spread(7)

    swap.before()

    @pl.when(step < blocks)
    def _():
        select_rows(tab_ref, idsb_ref, sel_ref)
        pre = dot_nt(tok_ref[...], sel_ref[...])
        gate = gate_ref[...]
        cdf = 0.5 * (1.0 + lax.erf(pre * 0.7071067811865476))
        pdf = jnp.exp(-0.5 * pre * pre) * 0.3989422804014327
        live = gate != 0.0
        w = jnp.where(live, gate * (pre * cdf), 0.0)
        w_ref[...] = w
        slope_ref[...] = jnp.where(live, gate * (cdf + pre * pdf), 0.0)
        one, two, three = split3(w)
        dyt = dyt_ref[...]
        grad_t = dot_nn(dyt, one) + dot_nn(dyt, two) + dot_nn(dyt, three)
        place_rows(step, grad_t, ids_ref, step % 2, swap.keep, swap.send)

    @pl.when(step == blocks + LAG - 1)
    def _():
        get_v.arrive(8)
        get_v.spread(8)

    swap.after()

    @pl.when(step == blocks + LAG - 1)
    def _():
        get_v.finish(6, 7, 8)


def first_pass(tok, dyt, table, idsb, ids_flip, gate, held):
    n_tok, width = tok.shape
    n_list = gate.shape[1]
    cols = OWN_STEP * 128
    steps = n_list // cols
    trows = table.shape[0] // steps
    at = lambda i: jnp.minimum(i, steps - 1)
    row_blk = pl.BlockSpec((cols, width), lambda i: (at(i), 0))
    mat_blk = pl.BlockSpec((n_tok, cols), lambda i: (0, at(i)))
    return pl.pallas_call(
        first_kernel,
        grid=(steps + LAG,),
        in_specs=[
            pl.BlockSpec((n_tok, width), lambda i: (0, 0)),
            pl.BlockSpec((width, n_tok), lambda i: (0, 0)),
            pl.BlockSpec((trows, width), lambda i: (at(i), 0)),
            pl.BlockSpec((cols, 128), lambda i: (at(i), 0)),
            pl.BlockSpec(ids_flip.shape, lambda i: (0, 0)),
            mat_blk,
            pl.BlockSpec(memory_space=pl.ANY),
        ],
        out_specs=[mat_blk, mat_blk, row_blk, pl.BlockSpec(memory_space=pl.ANY)] + Exchanger.out_specs(),
        out_shape=[
            jax.ShapeDtypeStruct((n_tok, n_list), F32),
            jax.ShapeDtypeStruct((n_tok, n_list), F32),
            jax.ShapeDtypeStruct((n_list, width), BF16),
            jax.ShapeDtypeStruct(held.shape, BF16),
        ] + Exchanger.out_shapes(width),
        scratch_shapes=Exchanger.scratch(width) + Gatherer.scratch(),
        input_output_aliases={6: 3},
        compiler_params=pltpu.CompilerParams(vmem_limit_bytes=VMEM_LIMIT, has_side_effects=True),
        cost_estimate=pl.CostEstimate(flops=11 * n_tok * n_list * width, bytes_accessed=n_list * (width * 10 + n_tok * 12), transcendentals=0),
        name="first_pass",
    )(tok, dyt, table, idsb, ids_flip, gate, held)


class Reducer(Ring):
    N_COPIES = 9

    @staticmethod
    def scratch(width):
        shapes = []
        for k in range(3):
            rows = ROW_CUTS[k + 1] - ROW_CUTS[k]
            lead = [(2, SIDE, SIDE), (2, SIDE, SIDE), (SIDE, SIDE), (2, SIDE), (SIDE,), (2,), (1,)]
            shapes += [pltpu.VMEM(dims + (rows, width), BF16) for dims in lead]
        return shapes + [pltpu.SemaphoreType.DMA((27,)), pltpu.SemaphoreType.DMA((27,)), pltpu.SemaphoreType.DMA((12,))]

    def __init__(self, src, first, out, scratch):
        super().__init__()
        self.src, self.first, self.out = src, first, out
        self.bufs = [scratch[7 * k:7 * k + 7] for k in range(3)]
        self.send_sem, self.recv_sem, self.load_sem = scratch[21:]

    def remote(self, k, num, src, dst, axis, first):
        at = k * self.N_COPIES + num
        return pltpu.make_async_remote_copy(src_ref=src, dst_ref=dst, send_sem=self.send_sem.at[at], recv_sem=self.recv_sem.at[at], device_id={'table': self.partner(axis, first)}, device_id_type=pl.DeviceIdType.MESH)

    def slab(self, k, slot):
        idx = [slice(None)] * 3
        idx[AXIS_ORDERS[k][0]] = slot
        return self.src.at[idx[0], idx[1], idx[2], pl.ds(ROW_CUTS[k], ROW_CUTS[k + 1] - ROW_CUTS[k])]

    def order(self, k, b, c):
        return (b, c) if AXIS_ORDERS[k][1] < AXIS_ORDERS[k][2] else (c, b)

    def loads(self):
        own = [pltpu.make_async_copy(self.slab(k, slot), self.bufs[k][0].at[j], self.load_sem.at[2 * k + j]) for j, slot in ((1, self.far), (0, 0)) for k in range(3)]
        come = [pltpu.make_async_copy(self.first[k].at[j], self.bufs[k][1].at[j], self.load_sem.at[6 + 2 * k + j]) for j in (1, 0) for k in range(3)]
        return [copy for j in range(2) for copy in own[3 * j:3 * j + 3] + come[3 * j:3 * j + 3]]

    def copies(self, stage):
        out = []
        for k in range(3):
            a, b, c = AXIS_ORDERS[k]
            held, got1, got2, got3, got4, got5, got6 = self.bufs[k]
            if stage == 2:
                out.append(self.remote(k, 2, held.at[1], got2, a, False))
            elif stage == 3:
                out += [self.remote(k, 3 + j, self.row_of(k, held, slot), got3.at[j], b, True) for j, slot in enumerate((self.near, 2))]
            elif stage == 4:
                out.append(self.remote(k, 5, self.row_of(k, held, self.far), got4, b, False))
            elif stage == 5:
                out += [self.remote(k, 6 + j, held.at[(0,) + self.order(k, 0, slot)], got5.at[j], c, True) for j, slot in enumerate((self.near, 2))]
            else:
                out.append(self.remote(k, 8, held.at[(0,) + self.order(k, 0, self.far)], got6.at[0], c, False))
        return out

    def row_of(self, k, held, slot):
        p, q = self.order(k, slot, slice(None))
        return held.at[0, p, q]

    def terms(self, k, b, c, depth):
        held, got1, got2, got3, got4, got5, got6 = self.bufs[k]
        p, q = self.order(k, b, c)
        arrs = [held[0, p, q], got1[0, p, q], got2[p, q]]
        return p, q, arrs

    def total(self, arrs):
        return functools.reduce(jnp.add, [arr.astype(F32) for arr in arrs])

    def add(self, stage):
        for k in range(3):
            held, got1, got2, got3, got4, got5, got6 = self.bufs[k]
            if stage == 2:
                def body(i, carry):
                    p, q = i // SIDE, i % SIDE
                    held[1, p, q] = self.total([held[1, p, q], got1[1, p, q]]).astype(BF16)
                    return carry
                lax.fori_loop(0, SIDE * SIDE, body, 0)
            elif stage == 3:
                def body(i, carry):
                    j = i // SIDE
                    p, q, arrs = self.terms(k, self.near + j * (2 - self.near), i % SIDE, 3)
                    held[0, p, q] = self.total(arrs).astype(BF16)
                    return carry
                lax.fori_loop(0, 2 * SIDE, body, 0)
            elif stage == 4:
                def body(c, carry):
                    p, q, arrs = self.terms(k, self.far, c, 4)
                    held[0, p, q] = self.total(arrs + [got3[1, c]]).astype(BF16)
                    return carry
                lax.fori_loop(0, SIDE, body, 0)
            elif stage == 5:
                for slot in (self.near, 2):
                    p, q, arrs = self.terms(k, 0, slot, 5)
                    held[0, p, q] = self.total(arrs + [got3[0, slot], got4[slot]]).astype(BF16)
            elif stage == 6:
                p, q, arrs = self.terms(k, 0, self.far, 6)
                held[0, p, q] = self.total(arrs + [got3[0, self.far], got4[self.far], got5[1]]).astype(BF16)
            else:
                p, q, arrs = self.terms(k, 0, 0, 7)
                self.out[ROW_CUTS[k]:ROW_CUTS[k + 1], :] = self.total(arrs + [got3[0, 0], got4[0], got5[0], got6[0]]).astype(self.out.dtype)

    def run(self, stage):
        if stage == 1:
            for copy in self.loads():
                copy.start()
            return
        if stage == 2:
            for copy in self.loads():
                copy.wait()
        else:
            for copy in self.copies(stage - 1):
                copy.wait_recv()
        self.add(stage)
        if stage < 7:
            for copy in self.copies(stage):
                copy.start()
        else:
            for done in range(2, 7):
                for copy in self.copies(done):
                    copy.wait_send()


def run_stages(reducer, step, last, marks):
    for stage, mark in marks:
        if last is None and mark is not None:
            pl.when(step == mark)(functools.partial(reducer.run, stage))
    if last is not None:
        @pl.when(step == last)
        def _():
            for stage, mark in marks:
                if mark is None:
                    reducer.run(stage)


SECOND_MARKS = ((1, 0), (2, 2), (3, 9), (4, 13), (5, 15), (6, 17), (7, None))
OUT_MARKS = ((1, 0), (2, 2), (3, 8), (4, 11), (5, 13), (6, 15), (7, None))


def second_kernel(dy_ref, tokt_ref, tab_ref, idsb_ref, ids_ref, slope_ref, part_ref, f0_ref, f1_ref, f2_ref, c_ref, sel_ref, *rest):
    step = pl.program_id(0)
    blocks = pl.num_programs(0) - LAG
    red_ref = rest[4]
    swap = Exchanger(step, blocks, rest[:4], rest[5:14])
    reducer = Reducer(part_ref, (f0_ref, f1_ref, f2_ref), red_ref, rest[14:])
    swap.before()
    run_stages(reducer, step, None, SECOND_MARKS)

    @pl.when(step < blocks)
    def _():
        select_rows(tab_ref, idsb_ref, sel_ref)
        back = dot_nt(dy_ref[...], sel_ref[...])
        slope = slope_ref[...]
        c = jnp.where(slope != 0.0, slope * back, 0.0)
        c_ref[...] = c
        one, two, three = split3(c)
        tokt = tokt_ref[...]
        grad_t = dot_nn(tokt, one) + dot_nn(tokt, two) + dot_nn(tokt, three)
        place_rows(step, grad_t, ids_ref, step % 2, swap.keep, swap.send)

    swap.after()
    run_stages(reducer, step, pl.num_programs(0) - 1, SECOND_MARKS)


def second_pass(dy, tokt, table, idsb, ids_flip, slope, part, first):
    n_tok, width = dy.shape
    n_list = slope.shape[1]
    cols = OWN_STEP * 128
    steps = n_list // cols
    trows = table.shape[0] // steps
    at = lambda i: jnp.minimum(i, steps - 1)
    row_blk = pl.BlockSpec((cols, width), lambda i: (at(i), 0))
    mat_blk = pl.BlockSpec((n_tok, cols), lambda i: (0, at(i)))
    return pl.pallas_call(
        second_kernel,
        grid=(steps + LAG,),
        in_specs=[
            pl.BlockSpec((n_tok, width), lambda i: (0, 0)),
            pl.BlockSpec((width, n_tok), lambda i: (0, 0)),
            pl.BlockSpec((trows, width), lambda i: (at(i), 0)),
            pl.BlockSpec((cols, 128), lambda i: (at(i), 0)),
            pl.BlockSpec(ids_flip.shape, lambda i: (0, 0)),
            mat_blk,
        ] + [pl.BlockSpec(memory_space=pl.ANY)] * 4,
        out_specs=[mat_blk, row_blk] + Exchanger.out_specs() + [pl.BlockSpec((128, width), lambda i: (0, 0))],
        out_shape=[
            jax.ShapeDtypeStruct((n_tok, n_list), F32),
            jax.ShapeDtypeStruct((n_list, width), BF16),
        ] + Exchanger.out_shapes(width) + [jax.ShapeDtypeStruct((128, width), BF16)],
        scratch_shapes=Exchanger.scratch(width) + Reducer.scratch(width),
        compiler_params=pltpu.CompilerParams(vmem_limit_bytes=VMEM_LIMIT, has_side_effects=True),
        cost_estimate=pl.CostEstimate(flops=11 * n_tok * n_list * width, bytes_accessed=n_list * (width * 10 + n_tok * 8), transcendentals=0),
        name="second_pass",
    )(dy, tokt, table, idsb, ids_flip, slope, part, *first)


def out_kernel(w_ref, v_ref, c_ref, u_ref, part_ref, f0_ref, f1_ref, f2_ref, y_ref, dx_ref, red_ref, y_acc, dx_acc, *scratch):
    step = pl.program_id(0)
    reducer = Reducer(part_ref, (f0_ref, f1_ref, f2_ref), red_ref, scratch)
    run_stages(reducer, step, None, OUT_MARKS)

    @pl.when(step == 0)
    def _():
        y_acc[...] = jnp.zeros_like(y_acc)
        dx_acc[...] = jnp.zeros_like(dx_acc)

    for mat_ref, row_ref, acc in ((w_ref, v_ref, y_acc), (c_ref, u_ref, dx_acc)):
        one, two, three = split3(mat_ref[...])
        rows = row_ref[...]
        acc[...] += dot_nn(one, rows) + dot_nn(two, rows) + dot_nn(three, rows)

    @pl.when(step == pl.num_programs(0) - 1)
    def _():
        y_ref[...] = y_acc[...].astype(y_ref.dtype)
        dx_ref[...] = dx_acc[...].astype(dx_ref.dtype)

    run_stages(reducer, step, pl.num_programs(0) - 1, OUT_MARKS)


def out_pass(w, v_sel, c, u_sel, part, first):
    n_tok, n_list = w.shape
    width = v_sel.shape[1]
    cols = 512
    mat_blk = pl.BlockSpec((n_tok, cols), lambda i: (0, i))
    row_blk = pl.BlockSpec((cols, width), lambda i: (i, 0))
    whole = pl.BlockSpec((n_tok, width), lambda i: (0, 0))
    return pl.pallas_call(
        out_kernel,
        grid=(n_list // cols,),
        in_specs=[mat_blk, row_blk, mat_blk, row_blk] + [pl.BlockSpec(memory_space=pl.ANY)] * 4,
        out_specs=[whole, whole, pl.BlockSpec((128, width), lambda i: (0, 0))],
        out_shape=[jax.ShapeDtypeStruct((n_tok, width), BF16)] * 2 + [jax.ShapeDtypeStruct((128, width), BF16)],
        scratch_shapes=[pltpu.VMEM((n_tok, width), F32)] * 2 + Reducer.scratch(width),
        compiler_params=pltpu.CompilerParams(vmem_limit_bytes=VMEM_LIMIT, has_side_effects=True),
        cost_estimate=pl.CostEstimate(flops=12 * n_tok * n_list * width, bytes_accessed=n_list * (width * 4 + n_tok * 8), transcendentals=0),
        name="out_pass",
    )(w, v_sel, c, u_sel, part, *first)


def solution(mesh):
    table_n = mesh.shape['table']
    tok_spec = P(('replica', 'data', 'table'))
    row_spec = P(('replica', 'table'))

    def device_step(tok, dy, u_loc, v_loc, wanted, pick, gate):
        n_local, width = u_loc.shape
        half = n_local // 2
        n_tok = tok.shape[0]
        core = lax.axis_index('data')
        me = lax.axis_index('table')
        owners = jnp.arange(table_n, dtype=jnp.int32) ^ me
        ids = jnp.take(wanted.reshape(table_n, -1), owners, axis=0, mode='clip') - owners[:, None] * n_local
        ids_flip = ids ^ (core * half)
        pick_rel = pick.reshape(n_tok, -1) ^ (me << 7)
        gates, idsb, full_u, full_v = gate_matrix(pick_rel, gate.reshape(n_tok, -1), ids, u_loc, v_loc, table_n)
        flat = lambda full: full.reshape(table_n * n_local, width)

        both_cores = lambda rows: lax.all_gather(rows, 'data', axis=0, tiled=True)
        w, slope, u_sel, full_v, part_v, *first_v = first_pass(tok, dy.T, flat(full_u), idsb, ids_flip, gates, full_v)
        c, v_sel, part_u, *first_u, red_v = second_pass(dy, tok.T, flat(full_v), idsb, ids_flip, slope, part_v, first_v)
        y, dx, red_u = out_pass(w, v_sel, c, u_sel, part_u, first_u)
        grad_v = both_cores(red_v)
        grad_u = both_cores(red_u)
        return y, dx, grad_u, grad_v

    return jax.shard_map(device_step, mesh=mesh, in_specs=(tok_spec, tok_spec, row_spec, row_spec, tok_spec, tok_spec, tok_spec), out_specs=(tok_spec, tok_spec, row_spec, row_spec), check_vma=False)
```

```python
import functools
import jax
import jax.numpy as jnp
from jax import lax
from jax.experimental import pallas as pl
from jax.experimental.pallas import tpu as pltpu
from jax.sharding import PartitionSpec as P

F32 = jnp.float32
BF16 = jnp.bfloat16
SIDE = 4
OWN_STEP = 4
VMEM_LIMIT = 60 * 1024 * 1024
ROW_CUTS = (0, 48, 88, 128)
AXIS_ORDERS = ((2, 1, 0), (1, 0, 2), (0, 2, 1))


def split3(val):
    one = val.astype(BF16)
    rest = val - one.astype(F32)
    two = rest.astype(BF16)
    rest = rest - two.astype(F32)
    return one, two, rest.astype(BF16)


def dot_nn(lhs, rhs):
    return lax.dot_general(lhs, rhs, (((1,), (0,)), ((), ())), preferred_element_type=F32)


def dot_nt(lhs, rhs):
    return lax.dot_general(lhs, rhs, (((1,), (1,)), ((), ())), preferred_element_type=F32)


def select_rows(tab_ref, idsb_ref, sel_ref):
    n_rows = tab_ref.shape[0] // OWN_STEP
    iota = lax.broadcasted_iota(jnp.int32, (128, 128), 1)
    for j in range(OWN_STEP):
        ids = idsb_ref[j * 128:(j + 1) * 128, :]
        hot = jnp.concatenate([jnp.where(ids == iota + 128 * h, 1.0, 0.0).astype(BF16) for h in range(n_rows // 128)], axis=1)
        sel_ref[j * 128:(j + 1) * 128, :] = dot_nn(hot, tab_ref[j * n_rows:(j + 1) * n_rows, :]).astype(BF16)


def place_rows(blk, grad_t, ids_ref, slot, keep_ref, send_ref):
    iota = lax.broadcasted_iota(jnp.int32, (256, 128), 0)
    grad_b = grad_t.astype(BF16)
    for j in range(OWN_STEP):
        hot = jnp.where(iota == ids_ref[pl.ds(blk * OWN_STEP + j, 1), :], 1.0, 0.0).astype(BF16)
        rows = dot_nt(hot, grad_b[:, j * 128:(j + 1) * 128]).astype(BF16)
        keep_ref[slot, j] = rows[:128]
        send_ref[slot, j] = rows[128:]


LAG = 3


class Exchanger:
    @staticmethod
    def scratch(width):
        blk = (2, OWN_STEP, 128, width)
        dma = pltpu.SemaphoreType.DMA
        return [pltpu.VMEM(blk, BF16)] * 4 + [dma((2,)), dma((2,)), dma((2,)), dma((6,)), dma((6,))]

    @staticmethod
    def out_shapes(width):
        rows = [ROW_CUTS[k + 1] - ROW_CUTS[k] for k in range(3)]
        cube = jax.ShapeDtypeStruct((SIDE, SIDE, SIDE, 128, width), BF16)
        return [cube] + [jax.ShapeDtypeStruct((2, SIDE, SIDE, n, width), BF16) for n in rows]

    @staticmethod
    def out_specs():
        return [pl.BlockSpec(memory_space=pl.ANY)] * 4

    def __init__(self, step, blocks, outs, scratch):
        self.step, self.blocks = step, blocks
        self.part_ref, self.first = outs[0], outs[1:]
        self.keep, self.send, self.got, self.sum = scratch[:4]
        self.pair_send, self.pair_recv, self.store_sem, self.out_send, self.out_recv = scratch[4:]
        self.ring = Ring()

    def pair_copy(self, slot):
        other = 1 - lax.axis_index('data')
        return pltpu.make_async_remote_copy(src_ref=self.send.at[slot], dst_ref=self.got.at[slot], send_sem=self.pair_send.at[slot], recv_sem=self.pair_recv.at[slot], device_id={'data': other}, device_id_type=pl.DeviceIdType.MESH)

    def store_copy(self, blk):
        slot = blk % 2
        return pltpu.make_async_copy(self.sum.at[slot], self.part_ref.at[blk // SIDE, blk % SIDE], self.store_sem.at[slot])

    def start_first(self, blk):
        spots = (blk // SIDE, blk % SIDE)
        near = self.ring.near
        for k in range(3):
            axis = AXIS_ORDERS[k][0]
            rows = pl.ds(ROW_CUTS[k], ROW_CUTS[k + 1] - ROW_CUTS[k])
            for way, mark in enumerate((near, 2)):
                def start(k=k, axis=axis, rows=rows, way=way, mark=mark):
                    if axis == 2:
                        src, dst = self.part_ref.at[spots[0], spots[1], mark, rows], self.first[k].at[way, spots[0], spots[1]]
                    else:
                        src, dst = self.part_ref.at[spots[0], spots[1], :, rows], self.first[k].at[way, spots[1 - axis]]
                    pltpu.make_async_remote_copy(src_ref=src, dst_ref=dst, send_sem=self.out_send.at[2 * k + way], recv_sem=self.out_recv.at[2 * k + way], device_id={'table': self.ring.partner(axis, True)}, device_id_type=pl.DeviceIdType.MESH).start()
                if axis == 2:
                    start()
                else:
                    pl.when(spots[axis] == mark)(start)

    def before(self):
        step, blocks = self.step, self.blocks

        @pl.when((step >= 3) & (step - 3 < blocks))
        def _():
            self.store_copy(step - 3).wait()
            self.start_first(step - 3)

        @pl.when((step >= 2) & (step - 2 < blocks))
        def _():
            slot = step % 2
            copy = self.pair_copy(slot)
            copy.wait_recv()
            for j in range(OWN_STEP):
                self.sum[slot, j] = self.keep[slot, j] + self.got[slot, j]
            self.store_copy(step - 2).start()
            copy.wait_send()

        @pl.when((step >= 1) & (step - 1 < blocks))
        def _():
            self.pair_copy((step - 1) % 2).start()

    def after(self):
        @pl.when(self.step == self.blocks + LAG - 1)
        def _():
            for k in range(3):
                for way in range(2):
                    dst = self.first[k].at[way]
                    pltpu.make_async_copy(dst, dst, self.out_send.at[2 * k + way]).wait()
                    pltpu.make_async_copy(dst, dst, self.out_recv.at[2 * k + way]).wait()


class Ring:
    def __init__(self):
        self.core = lax.axis_index('data')
        self.near, self.far = 1 + 2 * self.core, 3 - 2 * self.core

    def partner(self, axis, first):
        me = lax.axis_index('table')
        stride = SIDE ** (2 - axis)
        pos = (me // stride) % SIDE
        even, odd = pos + 1 - 2 * (pos % 2), 3 - pos
        new = even + self.core * (odd - even) if first else odd + self.core * (even - odd)
        return me + (new - pos) * stride


class Gatherer(Ring):
    STEPS = {1: (0,), 2: (1, 2), 3: (3,), 4: (4, 5), 5: (6,), 6: (7, 8)}

    @staticmethod
    def scratch():
        return [pltpu.SemaphoreType.DMA((27,))] * 4 + [pltpu.SemaphoreType.DMA((1,))]

    def __init__(self, own, full, scratch):
        super().__init__()
        self.own, self.full = own, full
        self.send_sem, self.recv_sem, self.pass_send, self.pass_recv, self.own_sem = scratch

    def spot(self, k, ia, ib, ic):
        idx = [None] * 3
        for axis, val in zip(AXIS_ORDERS[k], (ia, ib, ic)):
            idx[axis] = val
        start = pl.multiple_of(self.core * 128 + ROW_CUTS[k], 8)
        return self.full.at[idx[0], idx[1], idx[2], pl.ds(start, ROW_CUTS[k + 1] - ROW_CUTS[k])]

    def ends(self, num):
        near, far, every = self.near, self.far, slice(None)
        return (
            ((0, 0, 0), (near, 0, 0)),
            ((0, 0, 0), (far, 0, 0)),
            ((near, 0, 0), (2, 0, 0)),
            ((every, 0, 0), (every, near, 0)),
            ((every, 0, 0), (every, far, 0)),
            ((every, near, 0), (every, 2, 0)),
            ((every, every, 0), (every, every, near)),
            ((every, every, 0), (every, every, far)),
            ((every, every, near), (every, every, 2)),
        )[num]

    def copy(self, k, num):
        src, dst = self.ends(num)
        step = [key for key, nums in self.STEPS.items() if num in nums][0]
        at = 9 * k + num
        there = self.partner(AXIS_ORDERS[k][(step - 1) // 2], step % 2 == 1)
        return pltpu.make_async_remote_copy(src_ref=self.spot(k, *src), dst_ref=self.spot(k, *dst), send_sem=self.send_sem.at[at], recv_sem=self.recv_sem.at[at], device_id={'table': there}, device_id_type=pl.DeviceIdType.MESH)

    def forward(self, k, num):
        here = self.spot(k, *self.ends(num)[1])
        at = 9 * k + num
        return pltpu.make_async_remote_copy(src_ref=here, dst_ref=here, send_sem=self.pass_send.at[at], recv_sem=self.pass_recv.at[at], device_id={'data': 1 - self.core}, device_id_type=pl.DeviceIdType.MESH)

    def own_copy(self):
        return pltpu.make_async_copy(self.own, self.full.at[0, 0, 0], self.own_sem.at[0])

    def send(self, step):
        for k in range(3):
            for num in self.STEPS[step]:
                self.copy(k, num).start()

    def arrive(self, *nums):
        for k in range(3):
            for num in nums:
                self.copy(k, num).wait_recv()

    def spread(self, *nums):
        for k in range(3):
            for num in nums:
                self.forward(k, num).start()

    def finish(self, *nums):
        for k in range(3):
            for num in nums:
                self.copy(k, num).wait_send()
                self.forward(k, num).wait_send()
                self.forward(k, num).wait_recv()


GATE_STEPS = 16


def gate_kernel(n_own, pick_ref, gate_ref, ids_ref, u_ref, v_ref, out_ref, idsb_ref, full_u_ref, full_v_ref, tile_ref, *scratch):
    step = pl.program_id(0)
    get_u = Gatherer(u_ref, full_u_ref, scratch[:5])
    get_v = Gatherer(v_ref, full_v_ref, scratch[5:])

    @pl.when(step == 0)
    def _():
        for get in (get_u, get_v):
            get.own_copy().start()
        for get in (get_u, get_v):
            get.own_copy().wait()
            get.send(1)
        for got, then in (((0,), 2), ((1, 2), 3), ((3,), 4)):
            for get in (get_u, get_v):
                get.arrive(*got)
                get.send(then)
                get.spread(*got)
        get_u.arrive(4, 5)
        get_u.send(5)
        get_u.spread(4, 5)

    @pl.when(step == 2)
    def _():
        get_v.arrive(4, 5)
        get_v.spread(4, 5)

    @pl.when(step == 9)
    def _():
        get_u.arrive(6)
        get_u.send(6)
        get_u.spread(6)

    for j in range(OWN_STEP):
        row = ids_ref[pl.ds(step * OWN_STEP + j, 1), :].astype(F32)
        idsb_ref[j * 128:(j + 1) * 128, :] = jnp.transpose(jnp.broadcast_to(row, (128, 128))).astype(jnp.int32)

    sel = pick_ref.shape[1]
    iota_own = lax.broadcasted_iota(jnp.int32, (n_own, sel), 0)
    iota_lo = lax.broadcasted_iota(jnp.int32, (128, sel), 0)

    def body(grp, carry):
        base = pl.multiple_of(grp * 8, 8)
        pick = pick_ref[pl.ds(base, 8), :]
        hi = pick >> 7
        lo = pick & 127
        parts = [piece.astype(F32) for piece in split3(gate_ref[pl.ds(base, 8), :])]
        for j in range(8):
            mask = iota_own == hi[j:j + 1, :]
            left = jnp.concatenate([jnp.where(mask, piece[j:j + 1, :], 0.0).astype(BF16) for piece in parts], axis=0)
            right = jnp.where(iota_lo == lo[j:j + 1, :], 1.0, 0.0).astype(BF16)
            res = dot_nt(left, right)
            tile_ref[j * n_own:(j + 1) * n_own, :] = res[:n_own] + res[n_own:2 * n_own] + res[2 * n_own:]
        for o in range(n_own):
            out_ref[pl.ds(base, 8), o * 128:(o + 1) * 128] = tile_ref[pl.ds(o, 8, stride=n_own), :]
        return carry

    lax.fori_loop(0, pick_ref.shape[0] // 8, body, 0)

    @pl.when(step == GATE_STEPS - 1)
    def _():
        get_v.finish(0, 1, 2, 3, 4, 5)
        get_u.arrive(7)
        get_u.spread(7)
        get_u.arrive(8)
        get_u.spread(8)
        get_u.finish(0, 1, 2, 3, 4, 5, 6, 7, 8)


def gate_matrix(pick_rel, gate, ids, u_loc, v_loc, n_own):
    tok, sel = pick_rel.shape
    blk = tok // GATE_STEPS
    own = pl.BlockSpec(u_loc.shape, lambda i: (0, 0))
    full = jax.ShapeDtypeStruct((SIDE, SIDE, SIDE) + u_loc.shape, BF16)
    return pl.pallas_call(
        functools.partial(gate_kernel, n_own),
        grid=(GATE_STEPS,),
        in_specs=[pl.BlockSpec((blk, sel), lambda i: (i, 0)), pl.BlockSpec((blk, sel), lambda i: (i, 0)), pl.BlockSpec(ids.shape, lambda i: (0, 0)), own, own],
        out_specs=[pl.BlockSpec((blk, n_own * 128), lambda i: (i, 0)), pl.BlockSpec((OWN_STEP * 128, 128), lambda i: (i, 0))] + [pl.BlockSpec(memory_space=pl.ANY)] * 2,
        out_shape=[jax.ShapeDtypeStruct((tok, n_own * 128), F32), jax.ShapeDtypeStruct((n_own * 128, 128), jnp.int32), full, full],
        scratch_shapes=[pltpu.VMEM((8 * n_own, 128), F32)] + Gatherer.scratch() + Gatherer.scratch(),
        compiler_params=pltpu.CompilerParams(vmem_limit_bytes=VMEM_LIMIT, has_side_effects=True),
        cost_estimate=pl.CostEstimate(flops=2 * tok * 256 * 256 * 192, bytes_accessed=tok * n_own * 512, transcendentals=0),
        name="gate_matrix",
    )(pick_rel, gate, ids, u_loc, v_loc)


def first_kernel(tok_ref, dyt_ref, tab_ref, idsb_ref, ids_ref, gate_ref, held_ref, w_ref, slope_ref, sel_ref, full_ref, *rest):
    step = pl.program_id(0)
    blocks = pl.num_programs(0) - LAG
    swap = Exchanger(step, blocks, rest[:4], rest[4:13])
    get_v = Gatherer(None, full_ref, rest[13:])

    @pl.when(step == 0)
    def _():
        get_v.send(5)

    @pl.when(step == 4)
    def _():
        get_v.arrive(6)
        get_v.send(6)
        get_v.spread(6)

    @pl.when(step == 11)
    def _():
        get_v.arrive(7)
        get_v.spread(7)

    swap.before()

    @pl.when(step < blocks)
    def _():
        select_rows(tab_ref, idsb_ref, sel_ref)
        pre = dot_nt(tok_ref[...], sel_ref[...])
        gate = gate_ref[...]
        cdf = 0.5 * (1.0 + lax.erf(pre * 0.7071067811865476))
        pdf = jnp.exp(-0.5 * pre * pre) * 0.3989422804014327
        live = gate != 0.0
        w = jnp.where(live, gate * (pre * cdf), 0.0)
        w_ref[...] = w
        slope_ref[...] = jnp.where(live, gate * (cdf + pre * pdf), 0.0)
        one, two, three = split3(w)
        dyt = dyt_ref[...]
        grad_t = dot_nn(dyt, one) + dot_nn(dyt, two) + dot_nn(dyt, three)
        place_rows(step, grad_t, ids_ref, step % 2, swap.keep, swap.send)

    @pl.when(step == blocks + LAG - 1)
    def _():
        get_v.arrive(8)
        get_v.spread(8)

    swap.after()

    @pl.when(step == blocks + LAG - 1)
    def _():
        get_v.finish(6, 7, 8)


def first_pass(tok, dyt, table, idsb, ids_flip, gate, held):
    n_tok, width = tok.shape
    n_list = gate.shape[1]
    cols = OWN_STEP * 128
    steps = n_list // cols
    trows = table.shape[0] // steps
    at = lambda i: jnp.minimum(i, steps - 1)
    row_blk = pl.BlockSpec((cols, width), lambda i: (at(i), 0))
    mat_blk = pl.BlockSpec((n_tok, cols), lambda i: (0, at(i)))
    return pl.pallas_call(
        first_kernel,
        grid=(steps + LAG,),
        in_specs=[
            pl.BlockSpec((n_tok, width), lambda i: (0, 0)),
            pl.BlockSpec((width, n_tok), lambda i: (0, 0)),
            pl.BlockSpec((trows, width), lambda i: (at(i), 0)),
            pl.BlockSpec((cols, 128), lambda i: (at(i), 0)),
            pl.BlockSpec(ids_flip.shape, lambda i: (0, 0)),
            mat_blk,
            pl.BlockSpec(memory_space=pl.ANY),
        ],
        out_specs=[mat_blk, mat_blk, row_blk, pl.BlockSpec(memory_space=pl.ANY)] + Exchanger.out_specs(),
        out_shape=[
            jax.ShapeDtypeStruct((n_tok, n_list), F32),
            jax.ShapeDtypeStruct((n_tok, n_list), F32),
            jax.ShapeDtypeStruct((n_list, width), BF16),
            jax.ShapeDtypeStruct(held.shape, BF16),
        ] + Exchanger.out_shapes(width),
        scratch_shapes=Exchanger.scratch(width) + Gatherer.scratch(),
        input_output_aliases={6: 3},
        compiler_params=pltpu.CompilerParams(vmem_limit_bytes=VMEM_LIMIT, has_side_effects=True),
        cost_estimate=pl.CostEstimate(flops=11 * n_tok * n_list * width, bytes_accessed=n_list * (width * 10 + n_tok * 12), transcendentals=0),
        name="first_pass",
    )(tok, dyt, table, idsb, ids_flip, gate, held)


class Reducer(Ring):
    N_COPIES = 9

    @staticmethod
    def scratch(width):
        shapes = []
        for k in range(3):
            rows = ROW_CUTS[k + 1] - ROW_CUTS[k]
            lead = [(2, SIDE, SIDE), (2, SIDE, SIDE), (SIDE, SIDE), (2, SIDE), (SIDE,), (2,), (1,)]
            shapes += [pltpu.VMEM(dims + (rows, width), BF16) for dims in lead]
        return shapes + [pltpu.SemaphoreType.DMA((27,)), pltpu.SemaphoreType.DMA((27,)), pltpu.SemaphoreType.DMA((12,))]

    def __init__(self, src, first, out, scratch):
        super().__init__()
        self.src, self.first, self.out = src, first, out
        self.bufs = [scratch[7 * k:7 * k + 7] for k in range(3)]
        self.send_sem, self.recv_sem, self.load_sem = scratch[21:]

    def remote(self, k, num, src, dst, axis, first):
        at = k * self.N_COPIES + num
        return pltpu.make_async_remote_copy(src_ref=src, dst_ref=dst, send_sem=self.send_sem.at[at], recv_sem=self.recv_sem.at[at], device_id={'table': self.partner(axis, first)}, device_id_type=pl.DeviceIdType.MESH)

    def slab(self, k, slot):
        idx = [slice(None)] * 3
        idx[AXIS_ORDERS[k][0]] = slot
        return self.src.at[idx[0], idx[1], idx[2], pl.ds(ROW_CUTS[k], ROW_CUTS[k + 1] - ROW_CUTS[k])]

    def order(self, k, b, c):
        return (b, c) if AXIS_ORDERS[k][1] < AXIS_ORDERS[k][2] else (c, b)

    def loads(self):
        own = [pltpu.make_async_copy(self.slab(k, slot), self.bufs[k][0].at[j], self.load_sem.at[2 * k + j]) for j, slot in ((1, self.far), (0, 0)) for k in range(3)]
        come = [pltpu.make_async_copy(self.first[k].at[j], self.bufs[k][1].at[j], self.load_sem.at[6 + 2 * k + j]) for j in (1, 0) for k in range(3)]
        return [copy for j in range(2) for copy in own[3 * j:3 * j + 3] + come[3 * j:3 * j + 3]]

    def copies(self, stage):
        out = []
        for k in range(3):
            a, b, c = AXIS_ORDERS[k]
            held, got1, got2, got3, got4, got5, got6 = self.bufs[k]
            if stage == 2:
                out.append(self.remote(k, 2, held.at[1], got2, a, False))
            elif stage == 3:
                out += [self.remote(k, 3 + j, self.row_of(k, held, slot), got3.at[j], b, True) for j, slot in enumerate((self.near, 2))]
            elif stage == 4:
                out.append(self.remote(k, 5, self.row_of(k, held, self.far), got4, b, False))
            elif stage == 5:
                out += [self.remote(k, 6 + j, held.at[(0,) + self.order(k, 0, slot)], got5.at[j], c, True) for j, slot in enumerate((self.near, 2))]
            else:
                out.append(self.remote(k, 8, held.at[(0,) + self.order(k, 0, self.far)], got6.at[0], c, False))
        return out

    def row_of(self, k, held, slot):
        p, q = self.order(k, slot, slice(None))
        return held.at[0, p, q]

    def terms(self, k, b, c, depth):
        held, got1, got2, got3, got4, got5, got6 = self.bufs[k]
        p, q = self.order(k, b, c)
        arrs = [held[0, p, q], got1[0, p, q], got2[p, q]]
        return p, q, arrs

    def total(self, arrs):
        return functools.reduce(jnp.add, [arr.astype(F32) for arr in arrs])

    def add(self, stage):
        for k in range(3):
            held, got1, got2, got3, got4, got5, got6 = self.bufs[k]
            if stage == 2:
                def body(i, carry):
                    p, q = i // SIDE, i % SIDE
                    held[1, p, q] = self.total([held[1, p, q], got1[1, p, q]]).astype(BF16)
                    return carry
                lax.fori_loop(0, SIDE * SIDE, body, 0)
            elif stage == 3:
                def body(i, carry):
                    j = i // SIDE
                    p, q, arrs = self.terms(k, self.near + j * (2 - self.near), i % SIDE, 3)
                    held[0, p, q] = self.total(arrs).astype(BF16)
                    return carry
                lax.fori_loop(0, 2 * SIDE, body, 0)
            elif stage == 4:
                def body(c, carry):
                    p, q, arrs = self.terms(k, self.far, c, 4)
                    held[0, p, q] = self.total(arrs + [got3[1, c]]).astype(BF16)
                    return carry
                lax.fori_loop(0, SIDE, body, 0)
            elif stage == 5:
                for slot in (self.near, 2):
                    p, q, arrs = self.terms(k, 0, slot, 5)
                    held[0, p, q] = self.total(arrs + [got3[0, slot], got4[slot]]).astype(BF16)
            elif stage == 6:
                p, q, arrs = self.terms(k, 0, self.far, 6)
                held[0, p, q] = self.total(arrs + [got3[0, self.far], got4[self.far], got5[1]]).astype(BF16)
            else:
                p, q, arrs = self.terms(k, 0, 0, 7)
                self.out[ROW_CUTS[k]:ROW_CUTS[k + 1], :] = self.total(arrs + [got3[0, 0], got4[0], got5[0], got6[0]]).astype(self.out.dtype)

    def run(self, stage):
        if stage == 1:
            for copy in self.loads():
                copy.start()
            return
        if stage == 2:
            for copy in self.loads():
                copy.wait()
        else:
            for copy in self.copies(stage - 1):
                copy.wait_recv()
        self.add(stage)
        if stage < 7:
            for copy in self.copies(stage):
                copy.start()
        else:
            for done in range(2, 7):
                for copy in self.copies(done):
                    copy.wait_send()


def run_stages(reducer, step, last, marks):
    for stage, mark in marks:
        if last is None and mark is not None:
            pl.when(step == mark)(functools.partial(reducer.run, stage))
    if last is not None:
        @pl.when(step == last)
        def _():
            for stage, mark in marks:
                if mark is None:
                    reducer.run(stage)


SECOND_MARKS = ((1, 0), (2, 2), (3, 9), (4, 13), (5, 15), (6, 17), (7, None))
OUT_MARKS = ((1, 0), (2, 1), (3, 4), (4, 6), (5, 7), (6, None), (7, None))


def second_kernel(dy_ref, tokt_ref, tab_ref, idsb_ref, ids_ref, slope_ref, part_ref, f0_ref, f1_ref, f2_ref, c_ref, sel_ref, *rest):
    step = pl.program_id(0)
    blocks = pl.num_programs(0) - LAG
    red_ref = rest[4]
    swap = Exchanger(step, blocks, rest[:4], rest[5:14])
    reducer = Reducer(part_ref, (f0_ref, f1_ref, f2_ref), red_ref, rest[14:])
    swap.before()
    run_stages(reducer, step, None, SECOND_MARKS)

    @pl.when(step < blocks)
    def _():
        select_rows(tab_ref, idsb_ref, sel_ref)
        back = dot_nt(dy_ref[...], sel_ref[...])
        slope = slope_ref[...]
        c = jnp.where(slope != 0.0, slope * back, 0.0)
        c_ref[...] = c
        one, two, three = split3(c)
        tokt = tokt_ref[...]
        grad_t = dot_nn(tokt, one) + dot_nn(tokt, two) + dot_nn(tokt, three)
        place_rows(step, grad_t, ids_ref, step % 2, swap.keep, swap.send)

    swap.after()
    run_stages(reducer, step, pl.num_programs(0) - 1, SECOND_MARKS)


def second_pass(dy, tokt, table, idsb, ids_flip, slope, part, first):
    n_tok, width = dy.shape
    n_list = slope.shape[1]
    cols = OWN_STEP * 128
    steps = n_list // cols
    trows = table.shape[0] // steps
    at = lambda i: jnp.minimum(i, steps - 1)
    row_blk = pl.BlockSpec((cols, width), lambda i: (at(i), 0))
    mat_blk = pl.BlockSpec((n_tok, cols), lambda i: (0, at(i)))
    return pl.pallas_call(
        second_kernel,
        grid=(steps + LAG,),
        in_specs=[
            pl.BlockSpec((n_tok, width), lambda i: (0, 0)),
            pl.BlockSpec((width, n_tok), lambda i: (0, 0)),
            pl.BlockSpec((trows, width), lambda i: (at(i), 0)),
            pl.BlockSpec((cols, 128), lambda i: (at(i), 0)),
            pl.BlockSpec(ids_flip.shape, lambda i: (0, 0)),
            mat_blk,
        ] + [pl.BlockSpec(memory_space=pl.ANY)] * 4,
        out_specs=[mat_blk, row_blk] + Exchanger.out_specs() + [pl.BlockSpec((128, width), lambda i: (0, 0))],
        out_shape=[
            jax.ShapeDtypeStruct((n_tok, n_list), F32),
            jax.ShapeDtypeStruct((n_list, width), BF16),
        ] + Exchanger.out_shapes(width) + [jax.ShapeDtypeStruct((128, width), BF16)],
        scratch_shapes=Exchanger.scratch(width) + Reducer.scratch(width),
        compiler_params=pltpu.CompilerParams(vmem_limit_bytes=VMEM_LIMIT, has_side_effects=True),
        cost_estimate=pl.CostEstimate(flops=11 * n_tok * n_list * width, bytes_accessed=n_list * (width * 10 + n_tok * 8), transcendentals=0),
        name="second_pass",
    )(dy, tokt, table, idsb, ids_flip, slope, part, *first)


def out_kernel(w_ref, v_ref, c_ref, u_ref, part_ref, f0_ref, f1_ref, f2_ref, y_ref, dx_ref, red_ref, y_acc, dx_acc, *scratch):
    step = pl.program_id(0)
    reducer = Reducer(part_ref, (f0_ref, f1_ref, f2_ref), red_ref, scratch)
    run_stages(reducer, step, None, OUT_MARKS)

    @pl.when(step == 0)
    def _():
        y_acc[...] = jnp.zeros_like(y_acc)
        dx_acc[...] = jnp.zeros_like(dx_acc)

    for mat_ref, row_ref, acc in ((w_ref, v_ref, y_acc), (c_ref, u_ref, dx_acc)):
        one, two, three = split3(mat_ref[...])
        rows = row_ref[...]
        acc[...] += dot_nn(one, rows) + dot_nn(two, rows) + dot_nn(three, rows)

    @pl.when(step == pl.num_programs(0) - 1)
    def _():
        y_ref[...] = y_acc[...].astype(y_ref.dtype)
        dx_ref[...] = dx_acc[...].astype(dx_ref.dtype)

    run_stages(reducer, step, pl.num_programs(0) - 1, OUT_MARKS)


def out_pass(w, v_sel, c, u_sel, part, first):
    n_tok, n_list = w.shape
    width = v_sel.shape[1]
    cols = 1024
    mat_blk = pl.BlockSpec((n_tok, cols), lambda i: (0, i))
    row_blk = pl.BlockSpec((cols, width), lambda i: (i, 0))
    whole = pl.BlockSpec((n_tok, width), lambda i: (0, 0))
    return pl.pallas_call(
        out_kernel,
        grid=(n_list // cols,),
        in_specs=[mat_blk, row_blk, mat_blk, row_blk] + [pl.BlockSpec(memory_space=pl.ANY)] * 4,
        out_specs=[whole, whole, pl.BlockSpec((128, width), lambda i: (0, 0))],
        out_shape=[jax.ShapeDtypeStruct((n_tok, width), BF16)] * 2 + [jax.ShapeDtypeStruct((128, width), BF16)],
        scratch_shapes=[pltpu.VMEM((n_tok, width), F32)] * 2 + Reducer.scratch(width),
        compiler_params=pltpu.CompilerParams(vmem_limit_bytes=VMEM_LIMIT, has_side_effects=True),
        cost_estimate=pl.CostEstimate(flops=12 * n_tok * n_list * width, bytes_accessed=n_list * (width * 4 + n_tok * 8), transcendentals=0),
        name="out_pass",
    )(w, v_sel, c, u_sel, part, *first)


def solution(mesh):
    table_n = mesh.shape['table']
    tok_spec = P(('replica', 'data', 'table'))
    row_spec = P(('replica', 'table'))

    def device_step(tok, dy, u_loc, v_loc, wanted, pick, gate):
        n_local, width = u_loc.shape
        half = n_local // 2
        n_tok = tok.shape[0]
        core = lax.axis_index('data')
        me = lax.axis_index('table')
        owners = jnp.arange(table_n, dtype=jnp.int32) ^ me
        ids = jnp.take(wanted.reshape(table_n, -1), owners, axis=0, mode='clip') - owners[:, None] * n_local
        ids_flip = ids ^ (core * half)
        pick_rel = pick.reshape(n_tok, -1) ^ (me << 7)
        gates, idsb, full_u, full_v = gate_matrix(pick_rel, gate.reshape(n_tok, -1), ids, u_loc, v_loc, table_n)
        flat = lambda full: full.reshape(table_n * n_local, width)

        both_cores = lambda rows: lax.all_gather(rows, 'data', axis=0, tiled=True)
        w, slope, u_sel, full_v, part_v, *first_v = first_pass(tok, dy.T, flat(full_u), idsb, ids_flip, gates, full_v)
        c, v_sel, part_u, *first_u, red_v = second_pass(dy, tok.T, flat(full_v), idsb, ids_flip, slope, part_v, first_v)
        y, dx, red_u = out_pass(w, v_sel, c, u_sel, part_u, first_u)
        grad_v = both_cores(red_v)
        grad_u = both_cores(red_u)
        return y, dx, grad_u, grad_v

    return jax.shard_map(device_step, mesh=mesh, in_specs=(tok_spec, tok_spec, row_spec, row_spec, tok_spec, tok_spec, tok_spec), out_specs=(tok_spec, tok_spec, row_spec, row_spec), check_vma=False)
```
